32 devices in a mesh: seq: 8 (over z, x), head: 4 (over y, core).
Axes of the slice: x: 2, y: 2, z: 4, core: 2. Of those that a mesh axis runs over, the one named last changes fastest.
Arguments:
- queries: bfloat16 [8192, 4096], P('seq', 'head'), may hold values from -8 to 8
- key_rows: bfloat16 [8192, 4096], P('seq', 'head'), may hold values from -8 to 8
- value_rows: bfloat16 [8192, 4096], P('seq', 'head'), may hold values from -6 to 6
- random_owner: int32 [128, 3], P('seq'), may hold values from 0 to 7, all different within a row; in each aligned block of 16 rows (0 to 15, 16 to 31, ...) at most 8 rows name the same one
- random_local: int32 [128, 3], P('seq'), may hold values from 0 to 15
- output_weight: bfloat16 [4096, 4096], P('head'), may hold values from -0.09375 to 0.09375
Outputs:
- layer_output: bfloat16 [8192, 4096], P(('seq', 'head'))
The draws below stay inside these ranges and needn't reach their ends.
Inputs may be any that keep to these rules, and one draw needn't show every extreme that they name: `random_owner`: each row names 3 different owners. Among the rows of one device (16 aligned rows) no owner is named more than 8 times, and in some device's rows one owner is named exactly 8 times.
All inputs are finite; a program needn't handle non-finite values.
Results may differ from the reference program's by a relative error of at most 0.0052.
Values may be sent and summed in bfloat16 or wider, within the bound.
No kernel may reach another device: no remote copies, remote signals or barrier semaphores. Data moves between devices by JAX's collectives and lax.ppermute only.
A program may use at most 192 MiB of HBM per device.

```python
import math
import jax
import jax.numpy as jnp
import numpy as np
from jax import lax

D = 4096
HEADS = 32
HEAD_DIM = 128
BLOCK = 64
RANDOM = 3
GLOBAL = 128
NB_DEV = 16
CAP = 8
NBLK = 128
TOKENS = 8192
N_SEQ = 8


def query_key_pair(key):
    folded = jax.random.fold_in(key, 11)
    streams = jax.random.split(folded, 8)
    total_width = HEADS * HEAD_DIM
    row_ids = jnp.arange(TOKENS, dtype=jnp.int32)[:, None]
    query_scale = jnp.where(row_ids < GLOBAL, 3.0, 2.0)
    query_values = jax.random.normal(streams[0], (TOKENS, total_width), jnp.float32) * query_scale
    key_values = jax.random.normal(streams[1], (TOKENS, total_width), jnp.float32)
    return (jnp.clip(query_values, -8.0, 8.0), jnp.clip(key_values, -8.0, 8.0))


def draw_queries(key, part):
    return query_key_pair(key)[0].astype(jnp.bfloat16)


def draw_key_rows(key, part):
    return query_key_pair(key)[1].astype(jnp.bfloat16)


def with_ends(values, key, low, largest):
    longest = values.shape.index(max(values.shape))
    spots = []
    for shift in (0, 1):
        where = [jax.random.randint(jax.random.fold_in(key, axis), (), 0, length) for axis, length in enumerate(values.shape)]
        where[longest] = (where[longest] + shift) % values.shape[longest]
        spots.append(tuple(where))
    return values.at[spots[0]].set(low).at[spots[1]].set(largest)


def level_of(stream_key, extent, cuts, low, high):
    gain = 1.0
    for dim, shards_of in cuts:
        steps = jax.random.uniform(jax.random.fold_in(jax.random.fold_in(stream_key, 6), dim), (shards_of,), jnp.float32, low / len(cuts), high / len(cuts))
        gain = gain * jnp.repeat(jnp.exp(steps), extent[dim] // shards_of).reshape((-1,) + (1,) * (len(extent) - 1 - dim))
    return gain


def assign_block(rng, own, number, rows, amount, top, most, slope):
    order = jax.random.permutation(rng, amount)
    crowded, common = shares(amount, rows * top, most, slope, True), shares(amount, rows * top, most, slope, False)
    places = jnp.arange(amount)

    def named(tallies, turn):
        used = int((tallies > 0).sum())
        fixed = max(1, used // 4)
        passed = fixed + (places - fixed + turn * (used - fixed)) % max(1, amount - fixed)
        return jnp.zeros((amount,), jnp.int32).at[order[jnp.where(places < fixed, places, passed)]].set(jnp.asarray(tallies, jnp.int32))

    tallies = jnp.where(number % 4 == 0, named(crowded, number // 4), named(common, number - number // 4 - 1))
    mixed = jax.random.permutation(jax.random.fold_in(own, 3), amount)
    giver, taker = mixed[0:amount // 2 * 2:2], mixed[1:amount // 2 * 2:2]
    margin = jnp.minimum(tallies[giver] - 1, most - tallies[taker]) // 2
    margin = jnp.where((giver == order[0]) | (taker == order[0]) | (tallies[taker] == 0), 0, jnp.maximum(margin, 0))
    passed = jax.random.randint(jax.random.fold_in(own, 4), (amount // 2,), 0, 1 << 20) % (margin + 1)
    tallies = tallies.at[giver].add(-passed).at[taker].add(passed)
    labels = jnp.searchsorted(jnp.cumsum(tallies), jnp.arange(rows * top), side="right").astype(jnp.int32)
    listing = labels.reshape(top, rows).T
    listing = listing[jax.random.permutation(jax.random.fold_in(own, 1), rows)]
    turn = jax.random.randint(jax.random.fold_in(own, 2), (rows, 1), 0, top)
    return jnp.take_along_axis(listing, (jnp.arange(top)[None, :] + turn) % top, axis=1)


def shares(number_of, total, bound, slope, full):
    weights = [(1 << 20) // math.isqrt(grade ** slope) + 1 for grade in range(1, number_of + 1)]
    largest = bound if full else min(bound, max(-(-total // number_of), total * weights[0] // sum(weights)))
    least = 1 if total - largest >= number_of - 1 else 0
    counts, surplus = [largest] + [least] * (number_of - 1), total - largest - least * (number_of - 1)
    while surplus > 0:
        movable = [i for i in range(1, number_of) if counts[i] < largest] or [i for i in range(1, number_of) if counts[i] < bound]
        mass, budget = sum([weights[i] for i in movable]), surplus
        for i in movable:
            extra = min(bound - counts[i], max(1, budget * weights[i] // mass), surplus)
            counts[i] = counts[i] + extra
            surplus = surplus - extra
    return np.array(counts)


def noise(own_key, dims, spread, limit, cuts=(), kind=jnp.bfloat16):
    level = level_of(own_key, dims, cuts, -0.22, 0.18) if cuts else 1.0
    values = jax.random.normal(own_key, dims, jnp.float32) * spread * level
    return jnp.minimum(jnp.maximum(values, -limit), limit).astype(kind)


def setup_inputs(seed: int = 0) -> dict:
    arg_keys = jax.random.split(jax.random.key(seed), 7)
    queries = draw_queries(jax.random.fold_in(arg_keys[6], 71), 0)
    key_rows = draw_key_rows(jax.random.fold_in(arg_keys[6], 71), 0)
    value_rows = noise(arg_keys[2], (TOKENS, HEADS * HEAD_DIM), 1.0, 6.0, ((0, 8), (1, 4)))
    random_owner_keys = jax.random.split(jax.random.fold_in(arg_keys[3], 1), NBLK // NB_DEV)
    random_owner_turns = jax.random.permutation(jax.random.fold_in(arg_keys[3], 3), NBLK // NB_DEV)
    random_owner = jax.vmap(lambda own, number: assign_block(jax.random.fold_in(arg_keys[3], 2), own, number, NB_DEV, NBLK // NB_DEV, RANDOM, CAP, 2))(random_owner_keys, random_owner_turns).reshape((NBLK, RANDOM))
    random_local = with_ends(jax.random.randint(arg_keys[4], (NBLK, RANDOM), 0, NB_DEV), jax.random.fold_in(arg_keys[4], 1), 0, NB_DEV - 1).astype(jnp.int32)
    output_weight = noise(arg_keys[5], (HEADS * HEAD_DIM, D), (HEADS * HEAD_DIM) ** -0.5, 0.09375, ((0, 4),))
    return dict(queries=queries, key_rows=key_rows, value_rows=value_rows, random_owner=random_owner, random_local=random_local, output_weight=output_weight)


masked_score = -1e30


def sparse_block(block_index, queries, key_padded, value_padded, key_rows, value_rows, random_block):
    score_scale = HEAD_DIM ** -0.5
    first_row = block_index * BLOCK
    query_block = lax.dynamic_slice_in_dim(queries, first_row, BLOCK, 0)
    window_keys = lax.dynamic_slice_in_dim(key_padded, first_row, 3 * BLOCK, 0)
    window_values = lax.dynamic_slice_in_dim(value_padded, first_row, 3 * BLOCK, 0)
    picked = random_block[block_index]
    offsets = (picked[:, None] * BLOCK + jnp.arange(BLOCK, dtype=jnp.int32)[None, :]).reshape(-1).astype(jnp.int32)
    random_keys = jnp.take(key_rows, offsets, axis=0)
    random_values = jnp.take(value_rows, offsets, axis=0)
    listed_keys = jnp.concatenate([window_keys, random_keys, key_rows[:GLOBAL]], axis=0)
    listed_values = jnp.concatenate([window_values, random_values, value_rows[:GLOBAL]], axis=0)
    listed = listed_keys.shape[0]
    slot_number = jnp.arange(listed, dtype=jnp.int32) // BLOCK
    usable = jnp.logical_and(jnp.logical_or(slot_number != 0, block_index > 0), jnp.logical_or(slot_number != 2, block_index < NBLK - 1))
    query_heads = query_block.astype(jnp.float32).reshape(BLOCK, HEADS, HEAD_DIM)
    key_heads = listed_keys.astype(jnp.float32).reshape(listed, HEADS, HEAD_DIM)
    value_heads = listed_values.astype(jnp.float32).reshape(listed, HEADS, HEAD_DIM)
    scores = jnp.einsum("qhd,khd->hqk", query_heads, key_heads) * score_scale
    scores = jnp.where(usable[None, None, :], scores, masked_score)
    row_max = jnp.max(scores, axis=2, keepdims=True)
    weight = jnp.where(usable[None, None, :], jnp.exp(scores - row_max), 0.0)
    row_total = jnp.sum(weight, axis=2)
    rounded = lax.optimization_barrier(weight.astype(jnp.bfloat16)).astype(jnp.float32)
    context = jnp.einsum("hqk,khd->qhd", rounded, value_heads) / jnp.transpose(row_total)[:, :, None]
    return context.reshape(BLOCK, HEADS * HEAD_DIM).astype(jnp.bfloat16)


def segment_part(segment, global_query, key_rows, value_rows):
    segment_rows = NB_DEV * BLOCK
    score_scale = HEAD_DIM ** -0.5
    segment_keys = lax.dynamic_slice_in_dim(key_rows, segment * segment_rows, segment_rows, 0)
    segment_values = lax.dynamic_slice_in_dim(value_rows, segment * segment_rows, segment_rows, 0)
    query_heads = global_query.astype(jnp.float32).reshape(GLOBAL, HEADS, HEAD_DIM)
    key_heads = segment_keys.astype(jnp.float32).reshape(segment_rows, HEADS, HEAD_DIM)
    value_heads = segment_values.astype(jnp.float32).reshape(segment_rows, HEADS, HEAD_DIM)
    scores = jnp.einsum("qhd,khd->hqk", query_heads, key_heads) * score_scale
    row_max = jnp.max(scores, axis=2)
    weight = jnp.exp(scores - row_max[:, :, None])
    row_total = jnp.sum(weight, axis=2)
    rounded = lax.optimization_barrier(weight.astype(jnp.bfloat16)).astype(jnp.float32)
    partial_value = jnp.einsum("hqk,khd->hqd", rounded, value_heads)
    return row_max, row_total, partial_value


def reference(queries, key_rows, value_rows, random_owner, random_local, output_weight):
    random_block = (random_owner * NB_DEV + random_local).astype(jnp.int32)
    total_width = HEADS * HEAD_DIM
    zero_block = jnp.zeros((BLOCK, total_width), key_rows.dtype)
    key_padded = jnp.concatenate([zero_block, key_rows, zero_block], axis=0)
    value_padded = jnp.concatenate([zero_block, value_rows, zero_block], axis=0)

    def one_block(block_index):
        return sparse_block(block_index, queries, key_padded, value_padded, key_rows, value_rows, random_block)

    sparse = lax.map(one_block, jnp.arange(NBLK, dtype=jnp.int32)).reshape(TOKENS, total_width)
    global_query = queries[:GLOBAL]

    def one_segment(segment):
        return segment_part(segment, global_query, key_rows, value_rows)

    segment_max, segment_total, segment_acc = lax.map(one_segment, jnp.arange(N_SEQ, dtype=jnp.int32))
    overall_max = jnp.max(segment_max, axis=0)
    factor = jnp.exp(segment_max - overall_max[None])
    global_out = jnp.sum(factor[..., None] * segment_acc, axis=0) / jnp.sum(factor * segment_total, axis=0)[..., None]
    global_out = jnp.transpose(global_out, (1, 0, 2)).reshape(GLOBAL, total_width)
    attention = jnp.concatenate([global_out.astype(jnp.bfloat16), sparse[GLOBAL:]], axis=0)
    return jnp.dot(attention, output_weight, preferred_element_type=jnp.float32).astype(jnp.bfloat16)
```

```python
import math

import jax
import jax.numpy as jnp
from jax import lax
from jax.experimental import pallas as pl
from jax.experimental.pallas import tpu as pltpu
from jax.sharding import PartitionSpec as P

HEAD_DIM = 128
BLOCK = 64
RANDOM = 3
GLOBAL = 128


masked_score = -1e30


def padded(array, sides, width):
    for axis, dim in sides:
        peers, length = (lax.axis_size(axis), array.shape[dim])
        up = [(i, (i + 1) % peers) for i in range(peers - 1)]
        down = [(j, i) for i, j in up]
        last = lax.slice_in_dim(array, length - width, length, axis=dim)
        first = lax.slice_in_dim(array, 0, width, axis=dim)
        before = lax.ppermute(last, axis, up)
        after = lax.ppermute(first, axis, down)
        array = jnp.concatenate([before, array, after], axis=dim)
    return array


def from_root(block, axis, holder):
    block = jnp.where(lax.axis_index(axis) == holder, block, jnp.zeros_like(block))
    return lax.psum(block, axis)


def combined_all(array, axis, combine):
    everything = jax.tree.map(lambda part: lax.all_gather(part, axis), array)
    first = jax.tree.map(lambda part: part[0], everything)

    def lap(k, so_far):
        return combine(so_far, jax.tree.map(lambda part: part[k], everything))

    return lax.fori_loop(1, lax.axis_size(axis), lap, first)


def slot_table(owner_ids, local_ids, seq_count, slot_count):
    owner_hits = (owner_ids[:, None] == jnp.arange(seq_count, dtype=jnp.int32)[None, :]).astype(
        jnp.int32
    )
    earlier = jnp.cumsum(owner_hits, axis=0) - owner_hits
    slot_ids = jnp.sum(earlier * owner_hits, axis=1)
    slot_hits = (slot_ids[:, None] == jnp.arange(slot_count, dtype=jnp.int32)[None, :]).astype(
        jnp.int32
    )
    request_table = jnp.sum(
        (owner_hits * local_ids[:, None])[:, :, None] * slot_hits[:, None, :], axis=0
    )
    return (request_table, slot_ids)


def local_exchange(queries, key_rows, value_rows, random_owner, random_local, output_weight):
    seq_count = lax.axis_size("seq")
    seq_index = lax.axis_index("seq")
    token_count, width_here = queries.shape
    blocks_here = token_count // BLOCK
    heads_here = width_here // HEAD_DIM
    slot_count = max(2, 4 * blocks_here // seq_count)
    total_blocks = seq_count * blocks_here
    score_scale = HEAD_DIM ** (-0.5)
    key_blocks = key_rows.reshape(blocks_here, BLOCK, width_here)
    value_blocks = value_rows.reshape(blocks_here, BLOCK, width_here)
    edge_slots = 0
    owner_flat = random_owner.reshape(-1)
    local_flat = random_local.reshape(-1)
    request_table, slot_ids = slot_table(owner_flat, local_flat, seq_count, slot_count)
    wanted = lax.all_to_all(request_table, "seq", split_axis=0, concat_axis=0, tiled=True)
    sent_keys = jnp.take(key_blocks, wanted, axis=0)
    sent_values = jnp.take(value_blocks, wanted, axis=0)
    got_keys = lax.all_to_all(sent_keys, "seq", split_axis=0, concat_axis=0, tiled=True)
    got_values = lax.all_to_all(sent_values, "seq", split_axis=0, concat_axis=0, tiled=True)
    slot_width = slot_count + edge_slots
    flat_slots = owner_flat * slot_width + slot_ids
    random_keys = jnp.take(got_keys.reshape(-1, BLOCK, width_here), flat_slots, axis=0)
    random_values = jnp.take(got_values.reshape(-1, BLOCK, width_here), flat_slots, axis=0)
    edge_pairs = jnp.stack(
        [jnp.stack([key_blocks[0], value_blocks[0]]), jnp.stack([key_blocks[-1], value_blocks[-1]])]
    )
    widened = padded(edge_pairs, (("seq", 0),), 1)
    left_key, left_value = (widened[0, 0], widened[0, 1])
    right_key, right_value = (widened[3, 0], widened[3, 1])
    global_rows = jnp.stack([queries[:GLOBAL], key_rows[:GLOBAL], value_rows[:GLOBAL]])
    global_rows = from_root(global_rows, "seq", 0)
    global_query = global_rows[0].reshape(GLOBAL, heads_here, HEAD_DIM)
    key_heads = key_rows.reshape(token_count, heads_here, HEAD_DIM)
    value_heads = value_rows.reshape(token_count, heads_here, HEAD_DIM)
    scores = (
        jnp.einsum("qhd,khd->hqk", global_query, key_heads, preferred_element_type=jnp.float32)
        * score_scale
    )
    row_max = jnp.max(scores, axis=2)
    weight = jnp.exp(scores - row_max[:, :, None])
    row_total = jnp.sum(weight, axis=2)
    partial_value = jnp.einsum(
        "hqk,khd->hqd", weight.astype(jnp.bfloat16), value_heads, preferred_element_type=jnp.float32
    )

    def combine(left_part, right_part):
        joint_max = jnp.maximum(left_part[0], right_part[0])
        left_factor = jnp.exp(left_part[0] - joint_max)
        right_factor = jnp.exp(right_part[0] - joint_max)
        return (
            joint_max,
            left_part[1] * left_factor + right_part[1] * right_factor,
            left_part[2] * left_factor[:, :, None] + right_part[2] * right_factor[:, :, None],
        )

    row_max, row_total, partial_value = combined_all(
        (row_max, row_total, partial_value), "seq", combine
    )
    global_out = jnp.transpose(partial_value / row_total[:, :, None], (1, 0, 2)).reshape(
        GLOBAL, width_here
    )
    key_padded = jnp.concatenate([left_key[None], key_blocks, right_key[None]], axis=0)
    value_padded = jnp.concatenate([left_value[None], value_blocks, right_value[None]], axis=0)
    global_keys = global_rows[1].reshape(GLOBAL // BLOCK, BLOCK, width_here)
    global_values = global_rows[2].reshape(GLOBAL // BLOCK, BLOCK, width_here)
    group_size = math.gcd(blocks_here, max(1, 512 // BLOCK))
    group_count = blocks_here // group_size
    listed = (3 + RANDOM) * BLOCK + GLOBAL
    slot_number = jnp.arange(listed, dtype=jnp.int32) // BLOCK

    def attend(packed):
        number, query_group, key_group, value_group = packed
        block_ids = (
            seq_index * blocks_here + number * group_size + jnp.arange(group_size, dtype=jnp.int32)
        )
        near_keys = lax.dynamic_slice_in_dim(key_padded, number * group_size, group_size + 2, 0)
        near_values = lax.dynamic_slice_in_dim(value_padded, number * group_size, group_size + 2, 0)
        window_keys = jnp.stack([near_keys[:-2], near_keys[1:-1], near_keys[2:]], axis=1)
        window_values = jnp.stack([near_values[:-2], near_values[1:-1], near_values[2:]], axis=1)
        listed_keys = jnp.concatenate(
            [
                window_keys,
                key_group,
                jnp.broadcast_to(global_keys[None], (group_size,) + global_keys.shape),
            ],
            axis=1,
        )
        listed_values = jnp.concatenate(
            [
                window_values,
                value_group,
                jnp.broadcast_to(global_values[None], (group_size,) + global_values.shape),
            ],
            axis=1,
        )
        group_keys = listed_keys.reshape(group_size, listed, heads_here, HEAD_DIM)
        group_values = listed_values.reshape(group_size, listed, heads_here, HEAD_DIM)
        query_heads = query_group.reshape(group_size, BLOCK, heads_here, HEAD_DIM)
        block_scores = (
            jnp.einsum(
                "bqhd,bkhd->bhqk", query_heads, group_keys, preferred_element_type=jnp.float32
            )
            * score_scale
        )
        usable = jnp.logical_and(
            jnp.logical_or(slot_number[None, :] != 0, block_ids[:, None] > 0),
            jnp.logical_or(slot_number[None, :] != 2, block_ids[:, None] < total_blocks - 1),
        )
        usable_keys = usable[:, None, None, :]
        block_scores = jnp.where(usable_keys, block_scores, masked_score)
        block_max = jnp.max(block_scores, axis=3, keepdims=True)
        block_weight = jnp.where(usable_keys, jnp.exp(block_scores - block_max), 0.0)
        block_total = jnp.sum(block_weight, axis=3)
        context = jnp.einsum(
            "bhqk,bkhd->bqhd",
            block_weight.astype(jnp.bfloat16),
            group_values,
            preferred_element_type=jnp.float32,
        )
        context = context / jnp.transpose(block_total, (0, 2, 1))[:, :, :, None]
        return context.reshape(group_size * BLOCK, width_here).astype(jnp.bfloat16)

    numbers = jnp.arange(group_count, dtype=jnp.int32)
    query_groups = queries.reshape(group_count, group_size, BLOCK, width_here)
    random_key_groups = random_keys.reshape(group_count, group_size, RANDOM, BLOCK, width_here)
    random_value_groups = random_values.reshape(group_count, group_size, RANDOM, BLOCK, width_here)
    sparse = lax.map(
        attend, (numbers, query_groups, random_key_groups, random_value_groups)
    ).reshape(token_count, width_here)
    top_rows = jnp.where(seq_index == 0, global_out.astype(jnp.bfloat16), sparse[:GLOBAL])
    attention = jnp.concatenate([top_rows, sparse[GLOBAL:]], axis=0)
    summed = lax.psum_scatter(
        jnp.dot(attention, output_weight, preferred_element_type=jnp.float32),
        "head",
        scatter_dimension=0,
        tiled=True,
    )
    return summed.astype(jnp.bfloat16)


LOG2E = 1.4426950408889634
GATHER_LIMIT = 64 * 1024 * 1024
PAIRS = ((3, 3), (1, 1))


def ring_order(count):
    return list(range(0, count, 2)) + list(range(count - 1, 0, -2))


def ring_perms(count):
    ring = ring_order(count)
    forward = [(ring[i], ring[(i + 1) % count]) for i in range(count)]
    return forward, [(b, a) for a, b in forward]


def attention_chunk(params, queries, keys, values, first_head, heads, seq_count, head_count, names):
    token_count = queries.shape[0]
    blocks_here = token_count // BLOCK
    total = seq_count * token_count
    quarter = token_count // head_count
    window = 3 * BLOCK
    factor = HEAD_DIM ** (-0.5) * LOG2E
    total_blocks = total // BLOCK
    contract_last = (((1,), (1,)), ((), ()))
    contract_mid = (((1,), (0,)), ((), ()))

    def body(par, query_ref, *rest):
        key_refs = rest[:seq_count]
        value_refs = rest[seq_count : 2 * seq_count]
        outs = rest[2 * seq_count : 2 * seq_count + head_count]
        key_buf, value_buf, done, sems = rest[2 * seq_count + head_count :]
        step = pl.program_id(0)
        slot = lax.rem(step, 2)

        def copies(head, into):
            columns = pl.ds(pl.multiple_of(head * HEAD_DIM, HEAD_DIM), HEAD_DIM)
            out = []
            for number in range(seq_count):
                rows = pl.ds(pl.multiple_of(par[names["key"] + number] * token_count, token_count), token_count)
                out.append(
                    pltpu.make_async_copy(
                        key_refs[number].at[:, columns], key_buf.at[into, rows, :], sems.at[into, number]
                    )
                )
                rows = pl.ds(pl.multiple_of(par[names["value"] + number] * token_count, token_count), token_count)
                out.append(
                    pltpu.make_async_copy(
                        value_refs[number].at[:, columns],
                        value_buf.at[into, rows, :],
                        sems.at[into, seq_count + number],
                    )
                )
            return out

        @pl.when(step == 0)
        def _():
            for copy in copies(0, 0):
                copy.start()

        @pl.when(step + 1 < heads)
        def _():
            for copy in copies(step + 1, 1 - slot):
                copy.start()

        for copy in copies(step, slot):
            copy.wait()

        column = lax.broadcasted_iota(jnp.int32, (1, window), 1)
        seq_index = par[names["seq"]]

        def rows_of(buf, start, size):
            return buf[slot, pl.ds(pl.multiple_of(start, BLOCK), size), :]

        def one_block(number, _):
            block = seq_index * blocks_here + number
            start = jnp.clip((block - 1) * BLOCK, 0, total - window)
            spots = [par[names["random"] + number * RANDOM + r] for r in range(RANDOM)]

            def listed(buf):
                return jnp.concatenate(
                    [rows_of(buf, start, window)]
                    + [rows_of(buf, spot, BLOCK) for spot in spots]
                    + [buf[slot, 0:GLOBAL, :]],
                    axis=0,
                )

            here = pl.ds(pl.multiple_of(number * BLOCK, BLOCK), BLOCK)
            scores = lax.dot_general(
                query_ref[here, :], listed(key_buf), contract_last, preferred_element_type=jnp.float32
            )
            owner = start // BLOCK + column // BLOCK
            bias = jnp.where(jnp.abs(owner - block) > 1, masked_score, 0.0)
            scores = jnp.concatenate([scores[:, :window] + bias, scores[:, window:]], axis=1)
            top = jnp.max(scores, axis=1, keepdims=True)
            weight = jnp.exp2((scores - top) * factor)
            row_total = jnp.sum(weight, axis=1, keepdims=True)
            context = lax.dot_general(
                weight.astype(jnp.bfloat16), listed(value_buf), contract_mid, preferred_element_type=jnp.float32
            )
            done[here, :] = (context / row_total).astype(jnp.bfloat16)
            return 0

        lax.fori_loop(0, blocks_here, one_block, 0, unroll=2)

        @pl.when(seq_index == 0)
        def _():
            query = query_ref[0:GLOBAL, :]

            def segment(number, carry):
                top, row_total, context = carry
                start = number * token_count
                scores = lax.dot_general(
                    query, rows_of(key_buf, start, token_count), contract_last, preferred_element_type=jnp.float32
                )
                joint = jnp.maximum(top, jnp.max(scores, axis=1, keepdims=True))
                weight = jnp.exp2((scores - joint) * factor)
                old = jnp.exp2((top - joint) * factor)
                row_total = row_total * old + jnp.sum(weight, axis=1, keepdims=True)
                context = context * old + lax.dot_general(
                    weight.astype(jnp.bfloat16),
                    rows_of(value_buf, start, token_count),
                    contract_mid,
                    preferred_element_type=jnp.float32,
                )
                return joint, row_total, context

            top, row_total, context = lax.fori_loop(
                0,
                seq_count,
                segment,
                (
                    jnp.full((GLOBAL, 1), masked_score, jnp.float32),
                    jnp.zeros((GLOBAL, 1), jnp.float32),
                    jnp.zeros((GLOBAL, HEAD_DIM), jnp.float32),
                ),
            )
            done[0:GLOBAL, :] = (context / row_total).astype(jnp.bfloat16)

        for number in range(head_count):
            start = jnp.bitwise_xor(par[names["head"]], number) * quarter
            outs[number][...] = done[pl.ds(pl.multiple_of(start, quarter), quarter), :]

    flops = 4 * heads * token_count * 8 * BLOCK * HEAD_DIM
    return pl.pallas_call(
        body,
        grid_spec=pltpu.PrefetchScalarGridSpec(
            num_scalar_prefetch=1,
            grid=(heads,),
            in_specs=[pl.BlockSpec((token_count, HEAD_DIM), lambda h, par: (0, first_head + h))]
            + [pl.BlockSpec(memory_space=pl.ANY)] * (2 * seq_count),
            out_specs=[pl.BlockSpec((quarter, HEAD_DIM), lambda h, par: (0, h))] * head_count,
            scratch_shapes=[
                pltpu.VMEM((2, total, HEAD_DIM), jnp.bfloat16),
                pltpu.VMEM((2, total, HEAD_DIM), jnp.bfloat16),
                pltpu.VMEM((token_count, HEAD_DIM), jnp.bfloat16),
                pltpu.SemaphoreType.DMA((2, 2 * seq_count)),
            ],
        ),
        out_shape=[jax.ShapeDtypeStruct((quarter, heads * HEAD_DIM), jnp.bfloat16)] * head_count,
        compiler_params=pltpu.CompilerParams(dimension_semantics=("arbitrary",)),
        cost_estimate=pl.CostEstimate(flops=flops, bytes_accessed=2 * total * heads * HEAD_DIM * 2, transcendentals=0),
        name=f"attend_{first_head}",
    )(params, queries, *keys, *values)


def project(parts, weights, row_starts, tile=512):
    rows = parts[0][0].shape[0]
    depth, width = weights[0].shape
    chunks = len(row_starts)

    def body(*refs):
        part_refs = refs[: len(weights) * chunks]
        weight_refs = refs[len(weights) * chunks : -1]
        total = jnp.zeros((rows, tile), jnp.float32)
        for number, weight in enumerate(weight_refs):
            left = jnp.concatenate(
                [part_refs[number * chunks + c][...] for c in range(chunks)], axis=1
            )
            total = total + jnp.dot(left, weight[...], preferred_element_type=jnp.float32)
        refs[-1][...] = total.astype(jnp.bfloat16)

    flat = [part for group in parts for part in group]
    return pl.pallas_call(
        body,
        grid=(width // tile,),
        in_specs=[pl.BlockSpec(part.shape, lambda n: (0, 0)) for part in flat]
        + [pl.BlockSpec((depth, tile), lambda n: (0, n))] * len(weights),
        out_specs=pl.BlockSpec((rows, tile), lambda n: (0, n)),
        out_shape=jax.ShapeDtypeStruct((rows, width), jnp.bfloat16),
        compiler_params=pltpu.CompilerParams(dimension_semantics=("arbitrary",)),
        cost_estimate=pl.CostEstimate(
            flops=2 * rows * depth * len(weights) * width, bytes_accessed=2 * depth * len(weights) * width, transcendentals=0
        ),
        name="project",
    )(*flat, *weights)


def local_gather(queries, key_rows, value_rows, random_owner, random_local, output_weight):
    seq_count, head_count = lax.axis_size("seq"), lax.axis_size("head")
    token_count, width_here = queries.shape
    heads_here = width_here // HEAD_DIM
    seq_index, head_index = lax.axis_index("seq"), lax.axis_index("head")
    ring = ring_order(seq_count)
    place = jnp.sum(jnp.where(jnp.array(ring) == seq_index, jnp.arange(seq_count), 0))
    steps = jnp.arange(seq_count)
    ring_ids = jnp.array(ring, dtype=jnp.int32)
    key_owner = jnp.take(ring_ids, (place - steps) % seq_count)
    value_owner = jnp.take(ring_ids, (place + steps) % seq_count)
    spots = (random_owner * token_count + random_local * BLOCK).reshape(-1)
    params = jnp.concatenate(
        [jnp.stack([seq_index, head_index]), key_owner, value_owner, spots]
    ).astype(jnp.int32)
    names = {"seq": 0, "head": 1, "key": 2, "value": 2 + seq_count, "random": 2 + 2 * seq_count}
    forward, backward = ring_perms(seq_count)

    def swap(array, distance):
        return lax.ppermute(array, "head", [(i, i ^ distance) for i in range(head_count)])

    far_weight = swap(output_weight, 2)
    parts = [[] for _ in range(head_count)]
    row_starts = []
    weights = []
    first_head = 0
    gate = None
    for pair in PAIRS:
        sizes = [heads_here * size // 8 for size in pair]
        chains = []
        for size in sizes:
            columns = slice(first_head * HEAD_DIM, (first_head + size) * HEAD_DIM)
            key_part, value_part = key_rows[:, columns], value_rows[:, columns]
            if gate is not None:
                key_part, value_part, _ = lax.optimization_barrier((key_part, value_part, gate))
            chains.append((first_head, size, [key_part], [value_part]))
            row_starts.append(first_head)
            first_head += size
        for number in range(seq_count - 1):
            for _, _, keys, values in chains:
                keys.append(lax.ppermute(keys[-1], "seq", forward))
                values.append(lax.ppermute(values[-1], "seq", backward))
            if number == seq_count - 3:
                gate = (chains[0][2][-1], chains[0][3][-1])
                if pair is PAIRS[-1]:
                    far_weight, own_weight, _ = lax.optimization_barrier((far_weight, output_weight, gate))
                    weights = [output_weight, swap(own_weight, 1), far_weight, swap(far_weight, 1)]
        for head, size, keys, values in chains:
            outs = attention_chunk(
                params, queries, keys, values, head, size, seq_count, head_count, names
            )
            for distance, part in enumerate(outs):
                parts[distance].append(swap(part, distance) if distance else part)
    return project(parts, weights, row_starts)


def local(queries, key_rows, value_rows, *rest):
    gathered = 2 * lax.axis_size("seq") * key_rows.size * key_rows.dtype.itemsize
    form = local_gather if gathered <= GATHER_LIMIT else local_exchange
    return form(queries, key_rows, value_rows, *rest)


def solution(mesh):
    in_specs = (
        P("seq", "head"),
        P("seq", "head"),
        P("seq", "head"),
        P("seq", None),
        P("seq", None),
        P("head", None),
    )
    out_specs = P(("seq", "head"), None)
    return jax.shard_map(local, mesh=mesh, in_specs=in_specs, out_specs=out_specs, check_vma=False)
```

```python
import math

import jax
import jax.numpy as jnp
from jax import lax
from jax.experimental import pallas as pl
from jax.experimental.pallas import tpu as pltpu
from jax.sharding import PartitionSpec as P

HEAD_DIM = 128
BLOCK = 64
RANDOM = 3
GLOBAL = 128


masked_score = -1e30


def padded(array, sides, width):
    for axis, dim in sides:
        peers, length = (lax.axis_size(axis), array.shape[dim])
        up = [(i, (i + 1) % peers) for i in range(peers - 1)]
        down = [(j, i) for i, j in up]
        last = lax.slice_in_dim(array, length - width, length, axis=dim)
        first = lax.slice_in_dim(array, 0, width, axis=dim)
        before = lax.ppermute(last, axis, up)
        after = lax.ppermute(first, axis, down)
        array = jnp.concatenate([before, array, after], axis=dim)
    return array


def from_root(block, axis, holder):
    block = jnp.where(lax.axis_index(axis) == holder, block, jnp.zeros_like(block))
    return lax.psum(block, axis)


def combined_all(array, axis, combine):
    everything = jax.tree.map(lambda part: lax.all_gather(part, axis), array)
    first = jax.tree.map(lambda part: part[0], everything)

    def lap(k, so_far):
        return combine(so_far, jax.tree.map(lambda part: part[k], everything))

    return lax.fori_loop(1, lax.axis_size(axis), lap, first)


def slot_table(owner_ids, local_ids, seq_count, slot_count):
    owner_hits = (owner_ids[:, None] == jnp.arange(seq_count, dtype=jnp.int32)[None, :]).astype(
        jnp.int32
    )
    earlier = jnp.cumsum(owner_hits, axis=0) - owner_hits
    slot_ids = jnp.sum(earlier * owner_hits, axis=1)
    slot_hits = (slot_ids[:, None] == jnp.arange(slot_count, dtype=jnp.int32)[None, :]).astype(
        jnp.int32
    )
    request_table = jnp.sum(
        (owner_hits * local_ids[:, None])[:, :, None] * slot_hits[:, None, :], axis=0
    )
    return (request_table, slot_ids)


def local_exchange(queries, key_rows, value_rows, random_owner, random_local, output_weight):
    seq_count = lax.axis_size("seq")
    seq_index = lax.axis_index("seq")
    token_count, width_here = queries.shape
    blocks_here = token_count // BLOCK
    heads_here = width_here // HEAD_DIM
    slot_count = max(2, 4 * blocks_here // seq_count)
    total_blocks = seq_count * blocks_here
    score_scale = HEAD_DIM ** (-0.5)
    key_blocks = key_rows.reshape(blocks_here, BLOCK, width_here)
    value_blocks = value_rows.reshape(blocks_here, BLOCK, width_here)
    edge_slots = 0
    owner_flat = random_owner.reshape(-1)
    local_flat = random_local.reshape(-1)
    request_table, slot_ids = slot_table(owner_flat, local_flat, seq_count, slot_count)
    wanted = lax.all_to_all(request_table, "seq", split_axis=0, concat_axis=0, tiled=True)
    sent_keys = jnp.take(key_blocks, wanted, axis=0)
    sent_values = jnp.take(value_blocks, wanted, axis=0)
    got_keys = lax.all_to_all(sent_keys, "seq", split_axis=0, concat_axis=0, tiled=True)
    got_values = lax.all_to_all(sent_values, "seq", split_axis=0, concat_axis=0, tiled=True)
    slot_width = slot_count + edge_slots
    flat_slots = owner_flat * slot_width + slot_ids
    random_keys = jnp.take(got_keys.reshape(-1, BLOCK, width_here), flat_slots, axis=0)
    random_values = jnp.take(got_values.reshape(-1, BLOCK, width_here), flat_slots, axis=0)
    edge_pairs = jnp.stack(
        [jnp.stack([key_blocks[0], value_blocks[0]]), jnp.stack([key_blocks[-1], value_blocks[-1]])]
    )
    widened = padded(edge_pairs, (("seq", 0),), 1)
    left_key, left_value = (widened[0, 0], widened[0, 1])
    right_key, right_value = (widened[3, 0], widened[3, 1])
    global_rows = jnp.stack([queries[:GLOBAL], key_rows[:GLOBAL], value_rows[:GLOBAL]])
    global_rows = from_root(global_rows, "seq", 0)
    global_query = global_rows[0].reshape(GLOBAL, heads_here, HEAD_DIM)
    key_heads = key_rows.reshape(token_count, heads_here, HEAD_DIM)
    value_heads = value_rows.reshape(token_count, heads_here, HEAD_DIM)
    scores = (
        jnp.einsum("qhd,khd->hqk", global_query, key_heads, preferred_element_type=jnp.float32)
        * score_scale
    )
    row_max = jnp.max(scores, axis=2)
    weight = jnp.exp(scores - row_max[:, :, None])
    row_total = jnp.sum(weight, axis=2)
    partial_value = jnp.einsum(
        "hqk,khd->hqd", weight.astype(jnp.bfloat16), value_heads, preferred_element_type=jnp.float32
    )

    def combine(left_part, right_part):
        joint_max = jnp.maximum(left_part[0], right_part[0])
        left_factor = jnp.exp(left_part[0] - joint_max)
        right_factor = jnp.exp(right_part[0] - joint_max)
        return (
            joint_max,
            left_part[1] * left_factor + right_part[1] * right_factor,
            left_part[2] * left_factor[:, :, None] + right_part[2] * right_factor[:, :, None],
        )

    row_max, row_total, partial_value = combined_all(
        (row_max, row_total, partial_value), "seq", combine
    )
    global_out = jnp.transpose(partial_value / row_total[:, :, None], (1, 0, 2)).reshape(
        GLOBAL, width_here
    )
    key_padded = jnp.concatenate([left_key[None], key_blocks, right_key[None]], axis=0)
    value_padded = jnp.concatenate([left_value[None], value_blocks, right_value[None]], axis=0)
    global_keys = global_rows[1].reshape(GLOBAL // BLOCK, BLOCK, width_here)
    global_values = global_rows[2].reshape(GLOBAL // BLOCK, BLOCK, width_here)
    group_size = math.gcd(blocks_here, max(1, 512 // BLOCK))
    group_count = blocks_here // group_size
    listed = (3 + RANDOM) * BLOCK + GLOBAL
    slot_number = jnp.arange(listed, dtype=jnp.int32) // BLOCK

    def attend(packed):
        number, query_group, key_group, value_group = packed
        block_ids = (
            seq_index * blocks_here + number * group_size + jnp.arange(group_size, dtype=jnp.int32)
        )
        near_keys = lax.dynamic_slice_in_dim(key_padded, number * group_size, group_size + 2, 0)
        near_values = lax.dynamic_slice_in_dim(value_padded, number * group_size, group_size + 2, 0)
        window_keys = jnp.stack([near_keys[:-2], near_keys[1:-1], near_keys[2:]], axis=1)
        window_values = jnp.stack([near_values[:-2], near_values[1:-1], near_values[2:]], axis=1)
        listed_keys = jnp.concatenate(
            [
                window_keys,
                key_group,
                jnp.broadcast_to(global_keys[None], (group_size,) + global_keys.shape),
            ],
            axis=1,
        )
        listed_values = jnp.concatenate(
            [
                window_values,
                value_group,
                jnp.broadcast_to(global_values[None], (group_size,) + global_values.shape),
            ],
            axis=1,
        )
        group_keys = listed_keys.reshape(group_size, listed, heads_here, HEAD_DIM)
        group_values = listed_values.reshape(group_size, listed, heads_here, HEAD_DIM)
        query_heads = query_group.reshape(group_size, BLOCK, heads_here, HEAD_DIM)
        block_scores = (
            jnp.einsum(
                "bqhd,bkhd->bhqk", query_heads, group_keys, preferred_element_type=jnp.float32
            )
            * score_scale
        )
        usable = jnp.logical_and(
            jnp.logical_or(slot_number[None, :] != 0, block_ids[:, None] > 0),
            jnp.logical_or(slot_number[None, :] != 2, block_ids[:, None] < total_blocks - 1),
        )
        usable_keys = usable[:, None, None, :]
        block_scores = jnp.where(usable_keys, block_scores, masked_score)
        block_max = jnp.max(block_scores, axis=3, keepdims=True)
        block_weight = jnp.where(usable_keys, jnp.exp(block_scores - block_max), 0.0)
        block_total = jnp.sum(block_weight, axis=3)
        context = jnp.einsum(
            "bhqk,bkhd->bqhd",
            block_weight.astype(jnp.bfloat16),
            group_values,
            preferred_element_type=jnp.float32,
        )
        context = context / jnp.transpose(block_total, (0, 2, 1))[:, :, :, None]
        return context.reshape(group_size * BLOCK, width_here).astype(jnp.bfloat16)

    numbers = jnp.arange(group_count, dtype=jnp.int32)
    query_groups = queries.reshape(group_count, group_size, BLOCK, width_here)
    random_key_groups = random_keys.reshape(group_count, group_size, RANDOM, BLOCK, width_here)
    random_value_groups = random_values.reshape(group_count, group_size, RANDOM, BLOCK, width_here)
    sparse = lax.map(
        attend, (numbers, query_groups, random_key_groups, random_value_groups)
    ).reshape(token_count, width_here)
    top_rows = jnp.where(seq_index == 0, global_out.astype(jnp.bfloat16), sparse[:GLOBAL])
    attention = jnp.concatenate([top_rows, sparse[GLOBAL:]], axis=0)
    summed = lax.psum_scatter(
        jnp.dot(attention, output_weight, preferred_element_type=jnp.float32),
        "head",
        scatter_dimension=0,
        tiled=True,
    )
    return summed.astype(jnp.bfloat16)


LOG2E = 1.4426950408889634
LAYERS = 4
CHUNKS = (3, 4, 1)
LANES = 128
PIECE = 16
GROUP = 4
NEAR_GROUP = 8


CONTRACT_LAST = (((1,), (1,)), ((), ()))
CONTRACT_MID = (((1,), (0,)), ((), ()))
FACTOR = HEAD_DIM ** (-0.5) * LOG2E


def soft(queries, keys, values, biases=None):
    scores = [
        lax.dot_general(q, k, CONTRACT_LAST, preferred_element_type=jnp.float32)
        for q, k in zip(queries, keys)
    ]
    if biases is not None:
        scores = [score + bias for score, bias in zip(scores, biases)]
    tops = [jnp.max(score, axis=1, keepdims=True) for score in scores]
    weights = [jnp.exp2((score - top) * FACTOR) for score, top in zip(scores, tops)]
    totals = [jnp.sum(weight, axis=1, keepdims=True) for weight in weights]
    contexts = [
        lax.dot_general(w.astype(jnp.bfloat16), v, CONTRACT_MID, preferred_element_type=jnp.float32)
        for w, v in zip(weights, values)
    ]
    return list(zip(tops, totals, contexts))


def aligned(start, size=BLOCK):
    return pl.ds(pl.multiple_of(start, BLOCK), size)


def keep(stats, rows, count, step, top, total):
    lane = lax.broadcasted_iota(jnp.int32, (count, LANES), 1)
    both = jnp.where(lane < 3 * PIECE, top, total)
    stats[rows, :] = jnp.where(lane % PIECE == step, both, stats[rows, :])


def pieces(value, heads):
    lane = lax.broadcasted_iota(jnp.int32, value.shape, 1)
    high = value.astype(jnp.bfloat16).astype(jnp.float32)
    middle = (value - high).astype(jnp.bfloat16).astype(jnp.float32)
    turn = lane // PIECE % 3
    part = jnp.where(turn == 0, high, jnp.where(turn == 1, middle, value - high - middle))
    used = jnp.logical_and(lane % PIECE < heads, lane < 6 * PIECE)
    return jnp.where(used, part, 0.0).astype(jnp.bfloat16)


def unpieced(value, head):
    row = lax.broadcasted_iota(jnp.int32, (LANES, LANES), 0)
    mine = row % PIECE == head
    return [
        jnp.dot(
            value,
            jnp.where(jnp.logical_and(mine, row // (3 * PIECE) == side), 1.0, 0.0).astype(jnp.bfloat16),
            preferred_element_type=jnp.float32,
        )
        for side in range(2)
    ]


def near_attention(params, queries, key_rows, value_rows, before, after, tokens, total_blocks):
    token_count, width = queries.shape
    heads = width // HEAD_DIM
    blocks_here = token_count // BLOCK
    window = 3 * BLOCK

    def body(par, query_ref, key_ref, value_ref, before_ref, after_ref, token_ref, out_ref, piece_ref, wide, stats):
        step = pl.program_id(0)
        for side, ref in ((0, key_ref), (1, value_ref)):
            wide[side, 0:BLOCK, :] = before_ref[side]
            wide[side, BLOCK : BLOCK + token_count, :] = ref[...]
            wide[side, BLOCK + token_count : 2 * BLOCK + token_count, :] = after_ref[side]
        place = lax.broadcasted_iota(jnp.int32, (1, window + GLOBAL), 1) // BLOCK
        seq_index = par[0]

        def some_blocks(turn, _):
            numbers = [turn * NEAR_GROUP + i for i in range(NEAR_GROUP)]
            here = [aligned(number * BLOCK) for number in numbers]
            near = [aligned(number * BLOCK, window) for number in numbers]
            keys, values = (
                [jnp.concatenate([wide[side, rows, :], token_ref[side]], axis=0) for rows in near]
                for side in range(2)
            )
            blocks = [seq_index * blocks_here + number for number in numbers]
            biases = [
                jnp.where(
                    jnp.logical_or(
                        jnp.logical_and(place == 0, block == 0),
                        jnp.logical_and(place == 2, block == total_blocks - 1),
                    ),
                    masked_score,
                    0.0,
                )
                for block in blocks
            ]
            found = soft([query_ref[rows, :] for rows in here], keys, values, biases)
            for rows, block, (top, total, context) in zip(here, blocks, found):
                out_ref[rows, :] = context
                top = jnp.where(block < GLOBAL // BLOCK, masked_score, top)
                keep(stats, rows, BLOCK, step, top, total)
            return 0

        lax.fori_loop(0, blocks_here // NEAR_GROUP, some_blocks, 0)

        @pl.when(step == heads - 1)
        def _():
            piece_ref[...] = pieces(stats[...], heads)

    column = pl.BlockSpec((token_count, HEAD_DIM), lambda h, par: (0, h))
    edge = pl.BlockSpec((2, BLOCK, HEAD_DIM), lambda h, par: (0, 0, h))
    return pl.pallas_call(
        body,
        grid_spec=pltpu.PrefetchScalarGridSpec(
            num_scalar_prefetch=1,
            grid=(heads,),
            in_specs=[column, column, column, edge, edge, pl.BlockSpec((2, GLOBAL, HEAD_DIM), lambda h, par: (0, 0, h))],
            out_specs=[column, pl.BlockSpec((token_count, LANES), lambda h, par: (0, 0))],
            scratch_shapes=[
                pltpu.VMEM((2, token_count + 2 * BLOCK, HEAD_DIM), jnp.bfloat16),
                pltpu.VMEM((token_count, LANES), jnp.float32),
            ],
        ),
        out_shape=[
            jax.ShapeDtypeStruct((token_count, width), jnp.float32),
            jax.ShapeDtypeStruct((token_count, LANES), jnp.bfloat16),
        ],
        compiler_params=pltpu.CompilerParams(dimension_semantics=("arbitrary",)),
        cost_estimate=pl.CostEstimate(
            flops=4 * width * token_count * (window + GLOBAL), bytes_accessed=8 * token_count * width, transcendentals=0
        ),
        name="near",
    )(params, queries, key_rows, value_rows, before, after, tokens)


def column_attention(params, queries, pairs, names):
    width = queries[0].shape[1]
    token_count = pairs[0].shape[1]
    heads = width // HEAD_DIM
    blocks_here = token_count // BLOCK
    column_tokens = len(pairs) * token_count
    asked = RANDOM * BLOCK
    callers = len(queries)

    def body(par, *rest):
        query_refs = rest[:callers]
        pair_refs = rest[callers : callers + len(pairs)]
        outs = rest[callers + len(pairs) : 2 * callers + len(pairs)]
        buf, stats, sems = rest[2 * callers + len(pairs) :]
        step = pl.program_id(0)
        slot = lax.rem(step, 2)

        def copies(head, into):
            columns = pl.ds(pl.multiple_of(head * HEAD_DIM, HEAD_DIM), HEAD_DIM)
            return [
                pltpu.make_async_copy(
                    ref.at[:, :, columns],
                    buf.at[into, :, aligned(par[names["layer"] + number] * token_count, token_count), :],
                    sems.at[into, number],
                )
                for number, ref in enumerate(pair_refs)
            ]

        def work():
            @pl.when(step == 0)
            def _():
                for copy in copies(0, 0):
                    copy.start()

            @pl.when(step + 1 < heads)
            def _():
                for copy in copies(step + 1, 1 - slot):
                    copy.start()

            for copy in copies(step, slot):
                copy.wait()

            columns = pl.ds(pl.multiple_of(step * HEAD_DIM, HEAD_DIM), HEAD_DIM)
            place = lax.broadcasted_iota(jnp.int32, (1, asked), 1) // BLOCK

            def store(caller, rows, count, top, total, context):
                outs[caller][rows, columns] = context.astype(jnp.bfloat16)
                keep(stats.at[caller], rows, count, step, top, total)

            def some_blocks(turn, _):
                chosen = [(caller, turn * GROUP + i) for i in range(GROUP) for caller in range(callers)]
                here = [aligned(number * BLOCK) for _, number in chosen]
                places_of = [caller * blocks_here + number for caller, number in chosen]
                spots = [
                    [aligned(par[names["spots"] + at * RANDOM + r]) for r in range(RANDOM)] for at in places_of
                ]
                keys, values = (
                    [jnp.concatenate([buf[slot, side, spot, :] for spot in row], axis=0) for row in spots]
                    for side in range(2)
                )
                biases = [
                    jnp.where(place < par[names["counts"] + at], 0.0, masked_score) for at in places_of
                ]
                asked_by = [query_refs[caller][rows, :] for (caller, _), rows in zip(chosen, here)]
                found = soft(asked_by, keys, values, biases)
                for (caller, _), rows, part in zip(chosen, here, found):
                    store(caller, rows, BLOCK, *part)
                return 0

            lax.fori_loop(0, blocks_here // GROUP, some_blocks, 0)

            for caller in range(callers):

                @pl.when(par[names["device"] + caller] == 0)
                def _():
                    query = query_refs[caller][0:GLOBAL, :]
                    rows = [slice(n * token_count, (n + 1) * token_count) for n in range(len(pairs))]
                    keys, values = ([buf[slot, side, row, :] for row in rows] for side in range(2))
                    found = soft([query] * len(pairs), keys, values)
                    joint = found[0][0]
                    for part in found[1:]:
                        joint = jnp.maximum(joint, part[0])
                    shares = [jnp.exp2((part[0] - joint) * FACTOR) for part in found]
                    total = sum(part[1] * share for part, share in zip(found, shares))
                    context = sum(part[2] * share for part, share in zip(found, shares))
                    store(caller, slice(0, GLOBAL), GLOBAL, joint, total, context)

                @pl.when(step == heads - 1)
                def _():
                    outs[caller][:, width:] = pieces(stats[caller], heads)

        pl.when(par[names["inner"]] == 1)(work)

    return pl.pallas_call(
        body,
        grid_spec=pltpu.PrefetchScalarGridSpec(
            num_scalar_prefetch=1,
            grid=(heads,),
            in_specs=[pl.BlockSpec((token_count, HEAD_DIM), lambda h, par: (0, h))] * callers
            + [pl.BlockSpec(memory_space=pl.ANY)] * len(pairs),
            out_specs=[pl.BlockSpec((token_count, width + LANES), lambda h, par: (0, 0))] * callers,
            scratch_shapes=[
                pltpu.VMEM((2, 2, column_tokens, HEAD_DIM), jnp.bfloat16),
                pltpu.VMEM((callers, token_count, LANES), jnp.float32),
                pltpu.SemaphoreType.DMA((2, len(pairs))),
            ],
        ),
        out_shape=[jax.ShapeDtypeStruct((token_count, width + LANES), jnp.bfloat16)] * callers,
        compiler_params=pltpu.CompilerParams(dimension_semantics=("arbitrary",)),
        cost_estimate=pl.CostEstimate(
            flops=4 * width * token_count * callers * asked, bytes_accessed=4 * column_tokens * width, transcendentals=0
        ),
    )(params, *queries, *pairs)


def merge(params, near, near_lse, inner_pair, outer_pair, first_head, names, head_count):
    token_count = near.shape[0]
    width = inner_pair[0].shape[1] - LANES
    heads = width // HEAD_DIM
    quarter = token_count // head_count
    some = inner_pair + outer_pair

    def body(par, near_ref, lse_ref, *rest):
        parts = rest[: 2 * len(some)]
        outs = rest[2 * len(some) : -1]
        done = rest[-1]
        step = pl.program_id(0)

        def join(group):
            found = [unpieced(lse_ref[...], first_head + step) + [near_ref[...]]]
            for number in group:
                context = parts[2 * number][...].astype(jnp.float32)
                found.append(unpieced(parts[2 * number + 1][...], step) + [context])
            top = jnp.maximum(jnp.maximum(found[0][0], found[1][0]), found[2][0])
            shares = [jnp.exp2((part[0] - top) * FACTOR) for part in found]
            total = sum(part[1] * share for part, share in zip(found, shares))
            context = sum(part[2] * share for part, share in zip(found, shares))
            done[...] = (context / total).astype(jnp.bfloat16)

        pl.when(par[names["inner"]] == 1)(lambda: join((0, 1)))
        pl.when(par[names["inner"]] == 0)(lambda: join((2, 3)))
        for number in range(head_count):
            start = jnp.bitwise_xor(par[names["head"]], number) * quarter
            outs[number][...] = done[pl.ds(pl.multiple_of(start, quarter), quarter), :]

    part_specs = [
        pl.BlockSpec((token_count, HEAD_DIM), lambda h, par: (0, h)),
        pl.BlockSpec((token_count, LANES), lambda h, par: (0, heads)),
    ]
    return pl.pallas_call(
        body,
        grid_spec=pltpu.PrefetchScalarGridSpec(
            num_scalar_prefetch=1,
            grid=(heads,),
            in_specs=[
                pl.BlockSpec((token_count, HEAD_DIM), lambda h, par: (0, first_head + h)),
                pl.BlockSpec((token_count, LANES), lambda h, par: (0, 0)),
            ]
            + part_specs * len(some),
            out_specs=[pl.BlockSpec((quarter, HEAD_DIM), lambda h, par: (0, h))] * head_count,
            scratch_shapes=[pltpu.VMEM((token_count, HEAD_DIM), jnp.bfloat16)],
        ),
        out_shape=[jax.ShapeDtypeStruct((quarter, width), jnp.bfloat16)] * head_count,
        compiler_params=pltpu.CompilerParams(dimension_semantics=("arbitrary",)),
        cost_estimate=pl.CostEstimate(flops=64 * token_count * width, bytes_accessed=8 * token_count * width, transcendentals=0),
    )(params, near, near_lse, *[part for part in some for _ in range(2)])


def project(parts, weights, row_starts, tile=512):
    rows = parts[0][0].shape[0]
    depth, width = weights[0].shape
    chunks = len(row_starts)

    def body(*refs):
        part_refs = refs[: len(weights) * chunks]
        weight_refs = refs[len(weights) * chunks : -1]
        total = jnp.zeros((rows, tile), jnp.float32)
        for number, weight in enumerate(weight_refs):
            left = jnp.concatenate(
                [part_refs[number * chunks + c][...] for c in range(chunks)], axis=1
            )
            total = total + jnp.dot(left, weight[...], preferred_element_type=jnp.float32)
        refs[-1][...] = total.astype(jnp.bfloat16)

    flat = [part for group in parts for part in group]
    return pl.pallas_call(
        body,
        grid=(width // tile,),
        in_specs=[pl.BlockSpec(part.shape, lambda n: (0, 0)) for part in flat]
        + [pl.BlockSpec((depth, tile), lambda n: (0, n))] * len(weights),
        out_specs=pl.BlockSpec((rows, tile), lambda n: (0, n)),
        out_shape=jax.ShapeDtypeStruct((rows, width), jnp.bfloat16),
        compiler_params=pltpu.CompilerParams(dimension_semantics=("arbitrary",)),
        cost_estimate=pl.CostEstimate(
            flops=2 * rows * depth * len(weights) * width, bytes_accessed=2 * depth * len(weights) * width, transcendentals=0
        ),
        name="project",
    )(*flat, *weights)


def local_columns(queries, key_rows, value_rows, random_owner, random_local, output_weight):
    seq_count, head_count = lax.axis_size("seq"), lax.axis_size("head")
    token_count, width_here = queries.shape
    heads_here = width_here // HEAD_DIM
    blocks_here = token_count // BLOCK
    seq_index, head_index = lax.axis_index("seq"), lax.axis_index("head")
    layer, side = seq_index // 2, seq_index % 2
    last = LAYERS - 1
    inner = jnp.logical_and(layer > 0, layer < last)
    outer_layer = jnp.where(layer * 2 < last, 0, last)
    mirror = last - layer
    ends = ((0, 1), (last, last - 1))
    to_inner = [(2 * a + x, 2 * b + x) for a, b in ends for x in range(2)]
    to_inner_across = [(2 * a + x, 2 * b + 1 - x) for a, b in ends for x in range(2)]
    to_outer = [(b, a) for a, b in to_inner]
    to_outer_across = [(b, a) for a, b in to_inner_across]
    middle = [(2 * a + x, 2 * (last - a) + x) for _, a in ends for x in range(2)]
    across = [(2 * a + x, 2 * a + 1 - x) for _, a in ends for x in range(2)]

    def move(array, pairs):
        return lax.ppermute(array, "seq", pairs)

    def swap(array, distance):
        return lax.ppermute(array, "head", [(i, i ^ distance) for i in range(head_count)])

    last_block = jnp.stack([key_rows[-BLOCK:], value_rows[-BLOCK:]])
    first_block = jnp.stack([key_rows[:BLOCK], value_rows[:BLOCK]])
    before = move(last_block, [(i, i + 1) for i in range(seq_count - 1)])
    after = move(first_block, [(i + 1, i) for i in range(seq_count - 1)])
    tokens = jnp.stack([key_rows[:GLOBAL], value_rows[:GLOBAL]])
    hops = [[(0, 1)]] + [[(2 * z + x, 2 * z + 2 + x) for x in range(2)] for z in range(LAYERS - 1)]
    for pairs in hops:
        got = move(tokens, pairs)
        reached = jnp.any(jnp.array([b for _, b in pairs]) == seq_index)
        tokens = jnp.where(reached, got, tokens)

    far_weight = swap(output_weight, 2)
    near, near_lse = near_attention(
        seq_index.astype(jnp.int32).reshape(1), queries, key_rows, value_rows, before, after, tokens, seq_count * blocks_here
    )

    parts = [[] for _ in range(head_count)]
    first_head = 0
    moved = []
    for number, size in enumerate(CHUNKS):
        size = heads_here * size // sum(CHUNKS)
        columns = slice(first_head * HEAD_DIM, (first_head + size) * HEAD_DIM)
        pair = jnp.stack([key_rows[:, columns], value_rows[:, columns]])
        query = queries[:, columns]
        if number == 0:
            listed = jnp.concatenate([random_owner, random_local], axis=1).astype(queries.dtype)
            spare = (0, query.shape[1] - 2 * RANDOM)
            query = jnp.concatenate([query, jnp.pad(listed, ((0, 0), spare))], axis=0)
        outer_pair = move(pair, to_inner)
        mirror_pair = move(pair, middle)
        callers = [query, move(query, to_inner), move(query, across), move(query, to_inner_across)]
        mirror_outer = move(outer_pair, middle)
        moved.append((first_head, callers, [pair, outer_pair, mirror_pair, mirror_outer]))
        first_head += size
    tables = jnp.stack([asked[token_count:, : 2 * RANDOM] for asked in moved[0][1]]).astype(jnp.int32)
    owners, locals_of = tables[:, :, :RANDOM], tables[:, :, RANDOM:]
    spots = owners // 2 * token_count + locals_of * BLOCK
    here = (owners % 2 == side).astype(jnp.int32)
    rank = jnp.cumsum(here, axis=2) - 1
    packed = [
        jnp.sum(jnp.where(jnp.logical_and(here == 1, rank == r), spots, 0), axis=2) for r in range(RANDOM)
    ]
    outer_device = 2 * outer_layer + side
    head_line = [seq_index, head_index, inner]
    layers = [layer, outer_layer, mirror, last - outer_layer]
    devices = [seq_index, outer_device, seq_index + 1 - 2 * side, outer_device + 1 - 2 * side]
    params = jnp.concatenate(
        [
            jnp.stack([jnp.asarray(v, jnp.int32) for v in head_line + layers + devices]),
            jnp.stack(packed, axis=2).reshape(-1),
            jnp.sum(here, axis=2).reshape(-1),
        ]
    ).astype(jnp.int32)
    names = {"seq": 0, "head": 1, "inner": 2, "layer": 3, "device": 7, "spots": 11}
    names["counts"] = 11 + 4 * blocks_here * RANDOM

    for first, callers, pairs in moved:
        found = column_attention(params, callers, pairs, names)
        inner_pair = [found[0], move(found[2], across)]
        outer_pair = [move(found[1], to_outer), move(found[3], to_outer_across)]
        outs = merge(params, near, near_lse, inner_pair, outer_pair, first, names, head_count)
        for distance, part in enumerate(outs):
            parts[distance].append(swap(part, distance) if distance else part)
    weights = [output_weight, swap(output_weight, 1), far_weight, swap(far_weight, 1)]
    return project(parts, weights, moved)


def local(*arrays):
    if lax.axis_size("seq") != 2 * LAYERS:
        return local_exchange(*arrays)
    return local_columns(*arrays)


def solution(mesh):
    in_specs = (
        P("seq", "head"),
        P("seq", "head"),
        P("seq", "head"),
        P("seq", None),
        P("seq", None),
        P("head", None),
    )
    out_specs = P(("seq", "head"), None)
    return jax.shard_map(local, mesh=mesh, in_specs=in_specs, out_specs=out_specs, check_vma=False)
```

```python
import math

import jax
import jax.numpy as jnp
from jax import lax
from jax.experimental import pallas as pl
from jax.experimental.pallas import tpu as pltpu
from jax.sharding import PartitionSpec as P

HEAD_DIM = 128
BLOCK = 64
RANDOM = 3
GLOBAL = 128


masked_score = -1e30


def padded(array, sides, width):
    for axis, dim in sides:
        peers, length = (lax.axis_size(axis), array.shape[dim])
        up = [(i, (i + 1) % peers) for i in range(peers - 1)]
        down = [(j, i) for i, j in up]
        last = lax.slice_in_dim(array, length - width, length, axis=dim)
        first = lax.slice_in_dim(array, 0, width, axis=dim)
        before = lax.ppermute(last, axis, up)
        after = lax.ppermute(first, axis, down)
        array = jnp.concatenate([before, array, after], axis=dim)
    return array


def from_root(block, axis, holder):
    block = jnp.where(lax.axis_index(axis) == holder, block, jnp.zeros_like(block))
    return lax.psum(block, axis)


def combined_all(array, axis, combine):
    everything = jax.tree.map(lambda part: lax.all_gather(part, axis), array)
    first = jax.tree.map(lambda part: part[0], everything)

    def lap(k, so_far):
        return combine(so_far, jax.tree.map(lambda part: part[k], everything))

    return lax.fori_loop(1, lax.axis_size(axis), lap, first)


def slot_table(owner_ids, local_ids, seq_count, slot_count):
    owner_hits = (owner_ids[:, None] == jnp.arange(seq_count, dtype=jnp.int32)[None, :]).astype(
        jnp.int32
    )
    earlier = jnp.cumsum(owner_hits, axis=0) - owner_hits
    slot_ids = jnp.sum(earlier * owner_hits, axis=1)
    slot_hits = (slot_ids[:, None] == jnp.arange(slot_count, dtype=jnp.int32)[None, :]).astype(
        jnp.int32
    )
    request_table = jnp.sum(
        (owner_hits * local_ids[:, None])[:, :, None] * slot_hits[:, None, :], axis=0
    )
    return (request_table, slot_ids)


def local_exchange(queries, key_rows, value_rows, random_owner, random_local, output_weight):
    seq_count = lax.axis_size("seq")
    seq_index = lax.axis_index("seq")
    token_count, width_here = queries.shape
    blocks_here = token_count // BLOCK
    heads_here = width_here // HEAD_DIM
    slot_count = max(2, 4 * blocks_here // seq_count)
    total_blocks = seq_count * blocks_here
    score_scale = HEAD_DIM ** (-0.5)
    key_blocks = key_rows.reshape(blocks_here, BLOCK, width_here)
    value_blocks = value_rows.reshape(blocks_here, BLOCK, width_here)
    edge_slots = 0
    owner_flat = random_owner.reshape(-1)
    local_flat = random_local.reshape(-1)
    request_table, slot_ids = slot_table(owner_flat, local_flat, seq_count, slot_count)
    wanted = lax.all_to_all(request_table, "seq", split_axis=0, concat_axis=0, tiled=True)
    sent_keys = jnp.take(key_blocks, wanted, axis=0)
    sent_values = jnp.take(value_blocks, wanted, axis=0)
    got_keys = lax.all_to_all(sent_keys, "seq", split_axis=0, concat_axis=0, tiled=True)
    got_values = lax.all_to_all(sent_values, "seq", split_axis=0, concat_axis=0, tiled=True)
    slot_width = slot_count + edge_slots
    flat_slots = owner_flat * slot_width + slot_ids
    random_keys = jnp.take(got_keys.reshape(-1, BLOCK, width_here), flat_slots, axis=0)
    random_values = jnp.take(got_values.reshape(-1, BLOCK, width_here), flat_slots, axis=0)
    edge_pairs = jnp.stack(
        [jnp.stack([key_blocks[0], value_blocks[0]]), jnp.stack([key_blocks[-1], value_blocks[-1]])]
    )
    widened = padded(edge_pairs, (("seq", 0),), 1)
    left_key, left_value = (widened[0, 0], widened[0, 1])
    right_key, right_value = (widened[3, 0], widened[3, 1])
    global_rows = jnp.stack([queries[:GLOBAL], key_rows[:GLOBAL], value_rows[:GLOBAL]])
    global_rows = from_root(global_rows, "seq", 0)
    global_query = global_rows[0].reshape(GLOBAL, heads_here, HEAD_DIM)
    key_heads = key_rows.reshape(token_count, heads_here, HEAD_DIM)
    value_heads = value_rows.reshape(token_count, heads_here, HEAD_DIM)
    scores = (
        jnp.einsum("qhd,khd->hqk", global_query, key_heads, preferred_element_type=jnp.float32)
        * score_scale
    )
    row_max = jnp.max(scores, axis=2)
    weight = jnp.exp(scores - row_max[:, :, None])
    row_total = jnp.sum(weight, axis=2)
    partial_value = jnp.einsum(
        "hqk,khd->hqd", weight.astype(jnp.bfloat16), value_heads, preferred_element_type=jnp.float32
    )

    def combine(left_part, right_part):
        joint_max = jnp.maximum(left_part[0], right_part[0])
        left_factor = jnp.exp(left_part[0] - joint_max)
        right_factor = jnp.exp(right_part[0] - joint_max)
        return (
            joint_max,
            left_part[1] * left_factor + right_part[1] * right_factor,
            left_part[2] * left_factor[:, :, None] + right_part[2] * right_factor[:, :, None],
        )

    row_max, row_total, partial_value = combined_all(
        (row_max, row_total, partial_value), "seq", combine
    )
    global_out = jnp.transpose(partial_value / row_total[:, :, None], (1, 0, 2)).reshape(
        GLOBAL, width_here
    )
    key_padded = jnp.concatenate([left_key[None], key_blocks, right_key[None]], axis=0)
    value_padded = jnp.concatenate([left_value[None], value_blocks, right_value[None]], axis=0)
    global_keys = global_rows[1].reshape(GLOBAL // BLOCK, BLOCK, width_here)
    global_values = global_rows[2].reshape(GLOBAL // BLOCK, BLOCK, width_here)
    group_size = math.gcd(blocks_here, max(1, 512 // BLOCK))
    group_count = blocks_here // group_size
    listed = (3 + RANDOM) * BLOCK + GLOBAL
    slot_number = jnp.arange(listed, dtype=jnp.int32) // BLOCK

    def attend(packed):
        number, query_group, key_group, value_group = packed
        block_ids = (
            seq_index * blocks_here + number * group_size + jnp.arange(group_size, dtype=jnp.int32)
        )
        near_keys = lax.dynamic_slice_in_dim(key_padded, number * group_size, group_size + 2, 0)
        near_values = lax.dynamic_slice_in_dim(value_padded, number * group_size, group_size + 2, 0)
        window_keys = jnp.stack([near_keys[:-2], near_keys[1:-1], near_keys[2:]], axis=1)
        window_values = jnp.stack([near_values[:-2], near_values[1:-1], near_values[2:]], axis=1)
        listed_keys = jnp.concatenate(
            [
                window_keys,
                key_group,
                jnp.broadcast_to(global_keys[None], (group_size,) + global_keys.shape),
            ],
            axis=1,
        )
        listed_values = jnp.concatenate(
            [
                window_values,
                value_group,
                jnp.broadcast_to(global_values[None], (group_size,) + global_values.shape),
            ],
            axis=1,
        )
        group_keys = listed_keys.reshape(group_size, listed, heads_here, HEAD_DIM)
        group_values = listed_values.reshape(group_size, listed, heads_here, HEAD_DIM)
        query_heads = query_group.reshape(group_size, BLOCK, heads_here, HEAD_DIM)
        block_scores = (
            jnp.einsum(
                "bqhd,bkhd->bhqk", query_heads, group_keys, preferred_element_type=jnp.float32
            )
            * score_scale
        )
        usable = jnp.logical_and(
            jnp.logical_or(slot_number[None, :] != 0, block_ids[:, None] > 0),
            jnp.logical_or(slot_number[None, :] != 2, block_ids[:, None] < total_blocks - 1),
        )
        usable_keys = usable[:, None, None, :]
        block_scores = jnp.where(usable_keys, block_scores, masked_score)
        block_max = jnp.max(block_scores, axis=3, keepdims=True)
        block_weight = jnp.where(usable_keys, jnp.exp(block_scores - block_max), 0.0)
        block_total = jnp.sum(block_weight, axis=3)
        context = jnp.einsum(
            "bhqk,bkhd->bqhd",
            block_weight.astype(jnp.bfloat16),
            group_values,
            preferred_element_type=jnp.float32,
        )
        context = context / jnp.transpose(block_total, (0, 2, 1))[:, :, :, None]
        return context.reshape(group_size * BLOCK, width_here).astype(jnp.bfloat16)

    numbers = jnp.arange(group_count, dtype=jnp.int32)
    query_groups = queries.reshape(group_count, group_size, BLOCK, width_here)
    random_key_groups = random_keys.reshape(group_count, group_size, RANDOM, BLOCK, width_here)
    random_value_groups = random_values.reshape(group_count, group_size, RANDOM, BLOCK, width_here)
    sparse = lax.map(
        attend, (numbers, query_groups, random_key_groups, random_value_groups)
    ).reshape(token_count, width_here)
    top_rows = jnp.where(seq_index == 0, global_out.astype(jnp.bfloat16), sparse[:GLOBAL])
    attention = jnp.concatenate([top_rows, sparse[GLOBAL:]], axis=0)
    summed = lax.psum_scatter(
        jnp.dot(attention, output_weight, preferred_element_type=jnp.float32),
        "head",
        scatter_dimension=0,
        tiled=True,
    )
    return summed.astype(jnp.bfloat16)


LOG2E = 1.4426950408889634
LAYERS = 4
CHUNKS = (3, 3, 2)
LANES = 128
SPARE = 32
GROUP = 4
NEAR_GROUP = 8


CONTRACT_LAST = (((1,), (1,)), ((), ()))
CONTRACT_MID = (((1,), (0,)), ((), ()))
FACTOR = HEAD_DIM ** (-0.5) * LOG2E


def soft(queries, keys, values, biases=None):
    scores = [
        lax.dot_general(q, k, CONTRACT_LAST, preferred_element_type=jnp.float32)
        for q, k in zip(queries, keys)
    ]
    if biases is not None:
        scores = [score + bias for score, bias in zip(scores, biases)]
    tops = [jnp.max(score, axis=1, keepdims=True) for score in scores]
    weights = [jnp.exp2((score - top) * FACTOR) for score, top in zip(scores, tops)]
    totals = [jnp.sum(weight, axis=1, keepdims=True) for weight in weights]
    contexts = [
        lax.dot_general(w.astype(jnp.bfloat16), v, CONTRACT_MID, preferred_element_type=jnp.float32)
        for w, v in zip(weights, values)
    ]
    return list(zip(tops, totals, contexts))


def aligned(start, size=BLOCK):
    return pl.ds(pl.multiple_of(start, BLOCK), size)


def lane_of(shape):
    return lax.broadcasted_iota(jnp.int32, shape, 1)


def lanes_for(lane, span, head):
    mine = lane == head
    for part in range(1, 6):
        mine = jnp.logical_or(mine, lane == part * span + head)
    return mine


def keep(stats, rows, mine, is_top, top, total):
    stats[rows, :] = jnp.where(mine, jnp.where(is_top, top, total), stats[rows, :])


def pieces(value, span):
    lane = lane_of(value.shape)
    high = value.astype(jnp.bfloat16).astype(jnp.float32)
    middle = (value - high).astype(jnp.bfloat16).astype(jnp.float32)
    low = value - high - middle
    out = jnp.zeros_like(value)
    for part in range(6):
        here = jnp.logical_and(lane >= part * span, lane < (part + 1) * span)
        out = jnp.where(here, (high, middle, low)[part % 3], out)
    return out


def unpieced(value, span, head):
    row = lax.broadcasted_iota(jnp.int32, (value.shape[1], LANES), 0)
    mine = lanes_for(row, span, head)
    is_top = row < 3 * span
    return [
        jnp.dot(
            value,
            jnp.where(jnp.logical_and(mine, side), 1.0, 0.0).astype(jnp.bfloat16),
            preferred_element_type=jnp.float32,
        )
        for side in (is_top, jnp.logical_not(is_top))
    ]


def spare_places(token_count, heads):
    return [
        (token_count + n // heads * SPARE, n % heads * LANES, n * LANES) for n in range(token_count // LANES)
    ]


def spare_rows(token_count, heads):
    return -(-(token_count // LANES) // heads) * SPARE


def near_attention(params, queries, key_rows, value_rows, before, after, tokens, total_blocks):
    token_count, width = queries.shape
    heads = width // HEAD_DIM
    blocks_here = token_count // BLOCK
    window = 3 * BLOCK

    def body(par, query_ref, key_ref, value_ref, before_ref, after_ref, token_ref, out_ref, piece_ref, wide, stats):
        step = pl.program_id(0)
        for side, ref in ((0, key_ref), (1, value_ref)):
            wide[side, 0:BLOCK, :] = before_ref[side]
            wide[side, BLOCK : BLOCK + token_count, :] = ref[...]
            wide[side, BLOCK + token_count : 2 * BLOCK + token_count, :] = after_ref[side]
        place = lax.broadcasted_iota(jnp.int32, (1, window + GLOBAL), 1) // BLOCK
        seq_index = par[0]
        lane = lane_of((BLOCK, LANES))
        mine, is_top = lanes_for(lane, heads, step), lane < 3 * heads

        def some_blocks(turn, _):
            numbers = [turn * NEAR_GROUP + i for i in range(NEAR_GROUP)]
            here = [aligned(number * BLOCK) for number in numbers]
            near = [aligned(number * BLOCK, window) for number in numbers]
            keys, values = (
                [jnp.concatenate([wide[side, rows, :], token_ref[side]], axis=0) for rows in near]
                for side in range(2)
            )
            blocks = [seq_index * blocks_here + number for number in numbers]
            biases = [
                jnp.where(
                    jnp.logical_or(
                        jnp.logical_and(place == 0, block == 0),
                        jnp.logical_and(place == 2, block == total_blocks - 1),
                    ),
                    masked_score,
                    0.0,
                )
                for block in blocks
            ]
            found = soft([query_ref[rows, :] for rows in here], keys, values, biases)
            for rows, block, (top, total, context) in zip(here, blocks, found):
                out_ref[rows, :] = context
                top = jnp.where(block < GLOBAL // BLOCK, masked_score, top)
                keep(stats, rows, mine, is_top, top, total)
            return 0

        lax.fori_loop(0, blocks_here // NEAR_GROUP, some_blocks, 0)

        @pl.when(step == heads - 1)
        def _():
            piece_ref[...] = pieces(stats[...], heads).astype(jnp.bfloat16)

    column = pl.BlockSpec((token_count, HEAD_DIM), lambda h, par: (0, h))
    edge = pl.BlockSpec((2, BLOCK, HEAD_DIM), lambda h, par: (0, 0, h))
    return pl.pallas_call(
        body,
        grid_spec=pltpu.PrefetchScalarGridSpec(
            num_scalar_prefetch=1,
            grid=(heads,),
            in_specs=[column, column, column, edge, edge, pl.BlockSpec((2, GLOBAL, HEAD_DIM), lambda h, par: (0, 0, h))],
            out_specs=[column, pl.BlockSpec((token_count, LANES), lambda h, par: (0, 0))],
            scratch_shapes=[
                pltpu.VMEM((2, token_count + 2 * BLOCK, HEAD_DIM), jnp.bfloat16),
                pltpu.VMEM((token_count, LANES), jnp.float32),
            ],
        ),
        out_shape=[
            jax.ShapeDtypeStruct((token_count, width), jnp.float32),
            jax.ShapeDtypeStruct((token_count, LANES), jnp.bfloat16),
        ],
        compiler_params=pltpu.CompilerParams(dimension_semantics=("arbitrary",)),
        cost_estimate=pl.CostEstimate(
            flops=4 * width * token_count * (window + GLOBAL), bytes_accessed=8 * token_count * width, transcendentals=0
        ),
        name="near",
    )(params, queries, key_rows, value_rows, before, after, tokens)


def column_attention(params, queries, pairs, names):
    width = queries[0].shape[1]
    token_count = pairs[0].shape[1]
    heads = width // HEAD_DIM
    blocks_here = token_count // BLOCK
    column_tokens = len(pairs) * token_count
    asked = RANDOM * BLOCK
    callers = len(queries)
    rows_sent = token_count + spare_rows(token_count, heads)

    def body(par, *rest):
        query_refs = rest[:callers]
        pair_refs = rest[callers : callers + len(pairs)]
        outs = rest[callers + len(pairs) : 2 * callers + len(pairs)]
        buf, stats, sems = rest[2 * callers + len(pairs) :]
        step = pl.program_id(0)
        slot = lax.rem(step, 2)

        def copies(head, into):
            columns = pl.ds(pl.multiple_of(head * HEAD_DIM, HEAD_DIM), HEAD_DIM)
            return [
                pltpu.make_async_copy(
                    ref.at[:, :, columns],
                    buf.at[into, :, aligned(par[names["layer"] + number] * token_count, token_count), :],
                    sems.at[into, number],
                )
                for number, ref in enumerate(pair_refs)
            ]

        def work():
            @pl.when(step == 0)
            def _():
                for copy in copies(0, 0):
                    copy.start()

            @pl.when(step + 1 < heads)
            def _():
                for copy in copies(step + 1, 1 - slot):
                    copy.start()

            for copy in copies(step, slot):
                copy.wait()

            columns = pl.ds(pl.multiple_of(step * HEAD_DIM, HEAD_DIM), HEAD_DIM)
            place = lax.broadcasted_iota(jnp.int32, (1, asked), 1) // BLOCK

            masks = {}
            for count in (BLOCK, GLOBAL):
                lane = lane_of((count, LANES))
                masks[count] = lanes_for(lane, heads, step), lane < 3 * heads

            def store(caller, rows, count, top, total, context):
                outs[caller][rows, columns] = context.astype(jnp.bfloat16)
                keep(stats.at[caller], rows, *masks[count], top, total)

            def some_blocks(turn, _):
                chosen = [(caller, turn * GROUP + i) for i in range(GROUP) for caller in range(callers)]
                here = [aligned(number * BLOCK) for _, number in chosen]
                places_of = [caller * blocks_here + number for caller, number in chosen]
                spots = [
                    [aligned(par[names["spots"] + at * RANDOM + r]) for r in range(RANDOM)] for at in places_of
                ]
                keys, values = (
                    [jnp.concatenate([buf[slot, side, spot, :] for spot in row], axis=0) for row in spots]
                    for side in range(2)
                )
                biases = [
                    jnp.where(place < par[names["counts"] + at], 0.0, masked_score) for at in places_of
                ]
                asked_by = [query_refs[caller][rows, :] for (caller, _), rows in zip(chosen, here)]
                found = soft(asked_by, keys, values, biases)
                for (caller, _), rows, part in zip(chosen, here, found):
                    store(caller, rows, BLOCK, *part)
                return 0

            lax.fori_loop(0, blocks_here // GROUP, some_blocks, 0)

            def ends_of_line(caller):
                @pl.when(par[names["device"] + caller] == 0)
                def _():
                    query = query_refs[caller][0:GLOBAL, :]
                    rows = [slice(n * token_count, (n + 1) * token_count) for n in range(len(pairs))]
                    keys, values = ([buf[slot, side, row, :] for row in rows] for side in range(2))
                    found = soft([query] * len(pairs), keys, values)
                    joint = found[0][0]
                    for part in found[1:]:
                        joint = jnp.maximum(joint, part[0])
                    shares = [jnp.exp2((part[0] - joint) * FACTOR) for part in found]
                    total = sum(part[1] * share for part, share in zip(found, shares))
                    context = sum(part[2] * share for part, share in zip(found, shares))
                    store(caller, slice(0, GLOBAL), GLOBAL, joint, total, context)

            for caller in range(callers):
                if caller % 2:
                    ends_of_line(caller)

                @pl.when(step == heads - 1)
                def _():
                    for row, column, token in spare_places(token_count, heads):
                        part = jnp.transpose(pieces(stats[caller, token : token + LANES, :], heads))
                        outs[caller][row : row + SPARE, column : column + LANES] = part[:SPARE].astype(jnp.bfloat16)

        pl.when(par[names["inner"]] == 1)(work)

    return pl.pallas_call(
        body,
        grid_spec=pltpu.PrefetchScalarGridSpec(
            num_scalar_prefetch=1,
            grid=(heads,),
            in_specs=[pl.BlockSpec((token_count, HEAD_DIM), lambda h, par: (0, h))] * callers
            + [pl.BlockSpec(memory_space=pl.ANY)] * len(pairs),
            out_specs=[pl.BlockSpec((rows_sent, width), lambda h, par: (0, 0))] * callers,
            scratch_shapes=[
                pltpu.VMEM((2, 2, column_tokens, HEAD_DIM), jnp.bfloat16),
                pltpu.VMEM((callers, token_count, LANES), jnp.float32),
                pltpu.SemaphoreType.DMA((2, len(pairs))),
            ],
        ),
        out_shape=[jax.ShapeDtypeStruct((rows_sent, width), jnp.bfloat16)] * callers,
        compiler_params=pltpu.CompilerParams(dimension_semantics=("arbitrary",)),
        cost_estimate=pl.CostEstimate(
            flops=4 * width * token_count * callers * asked, bytes_accessed=4 * column_tokens * width, transcendentals=0
        ),
    )(params, *queries, *pairs)


def merge(params, near, near_lse, inner_pair, outer_pair, first_head, names, head_count):
    token_count = near.shape[0]
    rows_sent, width = inner_pair[0].shape
    heads = width // HEAD_DIM
    quarter = token_count // head_count
    some = inner_pair + outer_pair

    def body(par, near_ref, lse_ref, *rest):
        parts = rest[: len(some)]
        outs = rest[len(some) : -2]
        stats, done = rest[-2:]
        step = pl.program_id(0)

        def join(group):
            @pl.when(step == 0)
            def _():
                for side, number in enumerate(group):
                    for row, column, token in spare_places(token_count, heads):
                        part = parts[number][row : row + SPARE, column : column + LANES].astype(jnp.float32)
                        stats[side, token : token + LANES, :] = jnp.transpose(part)

            columns = pl.ds(pl.multiple_of(step * HEAD_DIM, HEAD_DIM), HEAD_DIM)
            all_heads = near.shape[1] // HEAD_DIM
            found = [unpieced(lse_ref[...], all_heads, first_head + step) + [near_ref[...]]]
            for side, number in enumerate(group):
                context = parts[number][0:token_count, columns].astype(jnp.float32)
                found.append(unpieced(stats[side].astype(jnp.bfloat16), heads, step) + [context])
            top = jnp.maximum(jnp.maximum(found[0][0], found[1][0]), found[2][0])
            shares = [jnp.exp2((part[0] - top) * FACTOR) for part in found]
            total = sum(part[1] * share for part, share in zip(found, shares))
            context = sum(part[2] * share for part, share in zip(found, shares))
            done[...] = (context / total).astype(jnp.bfloat16)

        pl.when(par[names["inner"]] == 1)(lambda: join((0, 1)))
        pl.when(par[names["inner"]] == 0)(lambda: join((2, 3)))
        for number in range(head_count):
            start = jnp.bitwise_xor(par[names["head"]], number) * quarter
            outs[number][...] = done[pl.ds(pl.multiple_of(start, quarter), quarter), :]

    return pl.pallas_call(
        body,
        grid_spec=pltpu.PrefetchScalarGridSpec(
            num_scalar_prefetch=1,
            grid=(heads,),
            in_specs=[
                pl.BlockSpec((token_count, HEAD_DIM), lambda h, par: (0, first_head + h)),
                pl.BlockSpec((token_count, LANES), lambda h, par: (0, 0)),
            ]
            + [pl.BlockSpec((rows_sent, width), lambda h, par: (0, 0))] * len(some),
            out_specs=[pl.BlockSpec((quarter, HEAD_DIM), lambda h, par: (0, h))] * head_count,
            scratch_shapes=[
                pltpu.VMEM((2, token_count, SPARE), jnp.float32),
                pltpu.VMEM((token_count, HEAD_DIM), jnp.bfloat16),
            ],
        ),
        out_shape=[jax.ShapeDtypeStruct((quarter, width), jnp.bfloat16)] * head_count,
        compiler_params=pltpu.CompilerParams(dimension_semantics=("arbitrary",)),
        cost_estimate=pl.CostEstimate(flops=64 * token_count * width, bytes_accessed=8 * token_count * width, transcendentals=0),
    )(params, near, near_lse, *some)


def project(parts, weights, tile=512):
    rows = parts[0][0].shape[0]
    width = weights[0].shape[1]
    chunks = len(parts[0])
    depth = sum(part.shape[1] for part in parts[0])
    sides = len(weights)

    def body(*refs):
        part_refs = refs[: sides * chunks]
        weight_refs = refs[sides * chunks : sides * chunks + sides]
        total = jnp.zeros((rows, tile), jnp.float32)
        for number, weight in enumerate(weight_refs):
            left = [part_refs[number * chunks + c][...] for c in range(chunks)]
            left = jnp.concatenate(left, axis=1)
            total = total + jnp.dot(left, weight[...], preferred_element_type=jnp.float32)
        refs[-1][...] = total.astype(refs[-1].dtype)

    flat = [part for group in parts for part in group]
    return pl.pallas_call(
        body,
        grid=(width // tile,),
        in_specs=[pl.BlockSpec(part.shape, lambda n: (0, 0)) for part in flat]
        + [pl.BlockSpec((depth, tile), lambda n: (0, n))] * sides,
        out_specs=pl.BlockSpec((rows, tile), lambda n: (0, n)),
        out_shape=jax.ShapeDtypeStruct((rows, width), jnp.bfloat16),
        compiler_params=pltpu.CompilerParams(dimension_semantics=("arbitrary",)),
        cost_estimate=pl.CostEstimate(
            flops=2 * rows * depth * sides * width, bytes_accessed=2 * depth * sides * width, transcendentals=0
        ),
        name="project",
    )(*flat, *weights)


def local_columns(queries, key_rows, value_rows, random_owner, random_local, output_weight):
    seq_count, head_count = lax.axis_size("seq"), lax.axis_size("head")
    token_count, width_here = queries.shape
    heads_here = width_here // HEAD_DIM
    blocks_here = token_count // BLOCK
    seq_index, head_index = lax.axis_index("seq"), lax.axis_index("head")
    layer, side = seq_index // 2, seq_index % 2
    last = LAYERS - 1
    inner = jnp.logical_and(layer > 0, layer < last)
    outer_layer = jnp.where(layer * 2 < last, 0, last)
    mirror = last - layer
    ends = ((0, 1), (last, last - 1))
    to_inner = [(2 * a + x, 2 * b + x) for a, b in ends for x in range(2)]
    to_outer = [(b, a) for a, b in to_inner]
    to_outer_across = [(2 * b + x, 2 * a + 1 - x) for a, b in ends for x in range(2)]
    middle = [(2 * a + x, 2 * (last - a) + x) for _, a in ends for x in range(2)]
    across = [(2 * a + x, 2 * a + 1 - x) for _, a in ends for x in range(2)]

    def move(array, pairs):
        return lax.ppermute(array, "seq", pairs)

    def swap(array, distance):
        return lax.ppermute(array, "head", [(i, i ^ distance) for i in range(head_count)])

    last_block = jnp.stack([key_rows[-BLOCK:], value_rows[-BLOCK:]])
    first_block = jnp.stack([key_rows[:BLOCK], value_rows[:BLOCK]])
    before = move(last_block, [(i, i + 1) for i in range(seq_count - 1)])
    after = move(first_block, [(i + 1, i) for i in range(seq_count - 1)])
    tokens = jnp.stack([key_rows[:GLOBAL], value_rows[:GLOBAL]])
    hops = [[(0, 1)]] + [[(2 * z + x, 2 * z + 2 + x) for x in range(2)] for z in range(LAYERS - 1)]
    for pairs in hops:
        got = move(tokens, pairs)
        reached = jnp.any(jnp.array([b for _, b in pairs]) == seq_index)
        tokens = jnp.where(reached, got, tokens)

    far_weight = swap(output_weight, 2)
    near, near_lse = near_attention(
        seq_index.astype(jnp.int32).reshape(1), queries, key_rows, value_rows, before, after, tokens, seq_count * blocks_here
    )

    parts = [[] for _ in range(head_count)]
    first_head = 0
    moved = []
    for number, size in enumerate(CHUNKS):
        size = heads_here * size // sum(CHUNKS)
        columns = slice(first_head * HEAD_DIM, (first_head + size) * HEAD_DIM)
        pair = jnp.stack([key_rows[:, columns], value_rows[:, columns]])
        query = queries[:, columns]
        if number == 0:
            listed = jnp.concatenate([random_owner, random_local], axis=1).astype(queries.dtype)
            spare = (0, query.shape[1] - 2 * RANDOM)
            query = jnp.concatenate([query, jnp.pad(listed, ((0, 0), spare))], axis=0)
        outer_pair = move(pair, to_inner)
        mirror_pair = move(pair, middle)
        from_outer = move(query, to_inner)
        from_side = move(query, across)
        callers = [query, from_outer, from_side, move(from_outer, across)]
        mirror_outer = move(outer_pair, middle)
        moved.append((first_head, callers, [pair, outer_pair, mirror_pair, mirror_outer]))
        first_head += size
    tables = jnp.stack([asked[token_count:, : 2 * RANDOM] for asked in moved[0][1]]).astype(jnp.int32)
    owners, locals_of = tables[:, :, :RANDOM], tables[:, :, RANDOM:]
    spots = owners // 2 * token_count + locals_of * BLOCK
    here = (owners % 2 == side).astype(jnp.int32)
    rank = jnp.cumsum(here, axis=2) - 1
    packed = [
        jnp.sum(jnp.where(jnp.logical_and(here == 1, rank == r), spots, 0), axis=2) for r in range(RANDOM)
    ]
    outer_device = 2 * outer_layer + side
    head_line = [seq_index, head_index, inner]
    layers = [layer, outer_layer, mirror, last - outer_layer]
    devices = [seq_index, outer_device, seq_index + 1 - 2 * side, outer_device + 1 - 2 * side]
    params = jnp.concatenate(
        [
            jnp.stack([jnp.asarray(v, jnp.int32) for v in head_line + layers + devices]),
            jnp.stack(packed, axis=2).reshape(-1),
            jnp.sum(here, axis=2).reshape(-1),
        ]
    ).astype(jnp.int32)
    names = {"seq": 0, "head": 1, "inner": 2, "layer": 3, "device": 7, "spots": 11}
    names["counts"] = 11 + 4 * blocks_here * RANDOM

    for first, callers, pairs in moved:
        found = column_attention(params, callers, pairs, names)
        inner_pair = [found[0], move(found[2], across)]
        outer_pair = [move(found[1], to_outer), move(found[3], to_outer_across)]
        outs = merge(params, near, near_lse, inner_pair, outer_pair, first, names, head_count)
        for distance, part in enumerate(outs):
            parts[distance].append(swap(part, distance) if distance else part)
    weights = [output_weight, swap(output_weight, 1), far_weight, swap(far_weight, 1)]
    return project(parts, weights)


def local(*arrays):
    if lax.axis_size("seq") != 2 * LAYERS:
        return local_exchange(*arrays)
    return local_columns(*arrays)


def solution(mesh):
    in_specs = (
        P("seq", "head"),
        P("seq", "head"),
        P("seq", "head"),
        P("seq", None),
        P("seq", None),
        P("head", None),
    )
    out_specs = P(("seq", "head"), None)
    return jax.shard_map(local, mesh=mesh, in_specs=in_specs, out_specs=out_specs, check_vma=False)
```

```python
import math

import jax
import jax.numpy as jnp
from jax import lax
from jax.experimental import pallas as pl
from jax.experimental.pallas import tpu as pltpu
from jax.sharding import PartitionSpec as P

HEAD_DIM = 128
BLOCK = 64
RANDOM = 3
GLOBAL = 128


masked_score = -1e30


def padded(array, sides, width):
    for axis, dim in sides:
        peers, length = (lax.axis_size(axis), array.shape[dim])
        up = [(i, (i + 1) % peers) for i in range(peers - 1)]
        down = [(j, i) for i, j in up]
        last = lax.slice_in_dim(array, length - width, length, axis=dim)
        first = lax.slice_in_dim(array, 0, width, axis=dim)
        before = lax.ppermute(last, axis, up)
        after = lax.ppermute(first, axis, down)
        array = jnp.concatenate([before, array, after], axis=dim)
    return array


def from_root(block, axis, holder):
    block = jnp.where(lax.axis_index(axis) == holder, block, jnp.zeros_like(block))
    return lax.psum(block, axis)


def combined_all(array, axis, combine):
    everything = jax.tree.map(lambda part: lax.all_gather(part, axis), array)
    first = jax.tree.map(lambda part: part[0], everything)

    def lap(k, so_far):
        return combine(so_far, jax.tree.map(lambda part: part[k], everything))

    return lax.fori_loop(1, lax.axis_size(axis), lap, first)


def slot_table(owner_ids, local_ids, seq_count, slot_count):
    owner_hits = (owner_ids[:, None] == jnp.arange(seq_count, dtype=jnp.int32)[None, :]).astype(
        jnp.int32
    )
    earlier = jnp.cumsum(owner_hits, axis=0) - owner_hits
    slot_ids = jnp.sum(earlier * owner_hits, axis=1)
    slot_hits = (slot_ids[:, None] == jnp.arange(slot_count, dtype=jnp.int32)[None, :]).astype(
        jnp.int32
    )
    request_table = jnp.sum(
        (owner_hits * local_ids[:, None])[:, :, None] * slot_hits[:, None, :], axis=0
    )
    return (request_table, slot_ids)


def local_exchange(queries, key_rows, value_rows, random_owner, random_local, output_weight):
    seq_count = lax.axis_size("seq")
    seq_index = lax.axis_index("seq")
    token_count, width_here = queries.shape
    blocks_here = token_count // BLOCK
    heads_here = width_here // HEAD_DIM
    slot_count = max(2, 4 * blocks_here // seq_count)
    total_blocks = seq_count * blocks_here
    score_scale = HEAD_DIM ** (-0.5)
    key_blocks = key_rows.reshape(blocks_here, BLOCK, width_here)
    value_blocks = value_rows.reshape(blocks_here, BLOCK, width_here)
    edge_slots = 0
    owner_flat = random_owner.reshape(-1)
    local_flat = random_local.reshape(-1)
    request_table, slot_ids = slot_table(owner_flat, local_flat, seq_count, slot_count)
    wanted = lax.all_to_all(request_table, "seq", split_axis=0, concat_axis=0, tiled=True)
    sent_keys = jnp.take(key_blocks, wanted, axis=0)
    sent_values = jnp.take(value_blocks, wanted, axis=0)
    got_keys = lax.all_to_all(sent_keys, "seq", split_axis=0, concat_axis=0, tiled=True)
    got_values = lax.all_to_all(sent_values, "seq", split_axis=0, concat_axis=0, tiled=True)
    slot_width = slot_count + edge_slots
    flat_slots = owner_flat * slot_width + slot_ids
    random_keys = jnp.take(got_keys.reshape(-1, BLOCK, width_here), flat_slots, axis=0)
    random_values = jnp.take(got_values.reshape(-1, BLOCK, width_here), flat_slots, axis=0)
    edge_pairs = jnp.stack(
        [jnp.stack([key_blocks[0], value_blocks[0]]), jnp.stack([key_blocks[-1], value_blocks[-1]])]
    )
    widened = padded(edge_pairs, (("seq", 0),), 1)
    left_key, left_value = (widened[0, 0], widened[0, 1])
    right_key, right_value = (widened[3, 0], widened[3, 1])
    global_rows = jnp.stack([queries[:GLOBAL], key_rows[:GLOBAL], value_rows[:GLOBAL]])
    global_rows = from_root(global_rows, "seq", 0)
    global_query = global_rows[0].reshape(GLOBAL, heads_here, HEAD_DIM)
    key_heads = key_rows.reshape(token_count, heads_here, HEAD_DIM)
    value_heads = value_rows.reshape(token_count, heads_here, HEAD_DIM)
    scores = (
        jnp.einsum("qhd,khd->hqk", global_query, key_heads, preferred_element_type=jnp.float32)
        * score_scale
    )
    row_max = jnp.max(scores, axis=2)
    weight = jnp.exp(scores - row_max[:, :, None])
    row_total = jnp.sum(weight, axis=2)
    partial_value = jnp.einsum(
        "hqk,khd->hqd", weight.astype(jnp.bfloat16), value_heads, preferred_element_type=jnp.float32
    )

    def combine(left_part, right_part):
        joint_max = jnp.maximum(left_part[0], right_part[0])
        left_factor = jnp.exp(left_part[0] - joint_max)
        right_factor = jnp.exp(right_part[0] - joint_max)
        return (
            joint_max,
            left_part[1] * left_factor + right_part[1] * right_factor,
            left_part[2] * left_factor[:, :, None] + right_part[2] * right_factor[:, :, None],
        )

    row_max, row_total, partial_value = combined_all(
        (row_max, row_total, partial_value), "seq", combine
    )
    global_out = jnp.transpose(partial_value / row_total[:, :, None], (1, 0, 2)).reshape(
        GLOBAL, width_here
    )
    key_padded = jnp.concatenate([left_key[None], key_blocks, right_key[None]], axis=0)
    value_padded = jnp.concatenate([left_value[None], value_blocks, right_value[None]], axis=0)
    global_keys = global_rows[1].reshape(GLOBAL // BLOCK, BLOCK, width_here)
    global_values = global_rows[2].reshape(GLOBAL // BLOCK, BLOCK, width_here)
    group_size = math.gcd(blocks_here, max(1, 512 // BLOCK))
    group_count = blocks_here // group_size
    listed = (3 + RANDOM) * BLOCK + GLOBAL
    slot_number = jnp.arange(listed, dtype=jnp.int32) // BLOCK

    def attend(packed):
        number, query_group, key_group, value_group = packed
        block_ids = (
            seq_index * blocks_here + number * group_size + jnp.arange(group_size, dtype=jnp.int32)
        )
        near_keys = lax.dynamic_slice_in_dim(key_padded, number * group_size, group_size + 2, 0)
        near_values = lax.dynamic_slice_in_dim(value_padded, number * group_size, group_size + 2, 0)
        window_keys = jnp.stack([near_keys[:-2], near_keys[1:-1], near_keys[2:]], axis=1)
        window_values = jnp.stack([near_values[:-2], near_values[1:-1], near_values[2:]], axis=1)
        listed_keys = jnp.concatenate(
            [
                window_keys,
                key_group,
                jnp.broadcast_to(global_keys[None], (group_size,) + global_keys.shape),
            ],
            axis=1,
        )
        listed_values = jnp.concatenate(
            [
                window_values,
                value_group,
                jnp.broadcast_to(global_values[None], (group_size,) + global_values.shape),
            ],
            axis=1,
        )
        group_keys = listed_keys.reshape(group_size, listed, heads_here, HEAD_DIM)
        group_values = listed_values.reshape(group_size, listed, heads_here, HEAD_DIM)
        query_heads = query_group.reshape(group_size, BLOCK, heads_here, HEAD_DIM)
        block_scores = (
            jnp.einsum(
                "bqhd,bkhd->bhqk", query_heads, group_keys, preferred_element_type=jnp.float32
            )
            * score_scale
        )
        usable = jnp.logical_and(
            jnp.logical_or(slot_number[None, :] != 0, block_ids[:, None] > 0),
            jnp.logical_or(slot_number[None, :] != 2, block_ids[:, None] < total_blocks - 1),
        )
        usable_keys = usable[:, None, None, :]
        block_scores = jnp.where(usable_keys, block_scores, masked_score)
        block_max = jnp.max(block_scores, axis=3, keepdims=True)
        block_weight = jnp.where(usable_keys, jnp.exp(block_scores - block_max), 0.0)
        block_total = jnp.sum(block_weight, axis=3)
        context = jnp.einsum(
            "bhqk,bkhd->bqhd",
            block_weight.astype(jnp.bfloat16),
            group_values,
            preferred_element_type=jnp.float32,
        )
        context = context / jnp.transpose(block_total, (0, 2, 1))[:, :, :, None]
        return context.reshape(group_size * BLOCK, width_here).astype(jnp.bfloat16)

    numbers = jnp.arange(group_count, dtype=jnp.int32)
    query_groups = queries.reshape(group_count, group_size, BLOCK, width_here)
    random_key_groups = random_keys.reshape(group_count, group_size, RANDOM, BLOCK, width_here)
    random_value_groups = random_values.reshape(group_count, group_size, RANDOM, BLOCK, width_here)
    sparse = lax.map(
        attend, (numbers, query_groups, random_key_groups, random_value_groups)
    ).reshape(token_count, width_here)
    top_rows = jnp.where(seq_index == 0, global_out.astype(jnp.bfloat16), sparse[:GLOBAL])
    attention = jnp.concatenate([top_rows, sparse[GLOBAL:]], axis=0)
    summed = lax.psum_scatter(
        jnp.dot(attention, output_weight, preferred_element_type=jnp.float32),
        "head",
        scatter_dimension=0,
        tiled=True,
    )
    return summed.astype(jnp.bfloat16)


LOG2E = 1.4426950408889634
LAYERS = 4
CHUNKS = (3, 3, 2)
LANES = 128
SPARE = 32
GROUP = 4
NEAR_GROUP = 8


CONTRACT_LAST = (((1,), (1,)), ((), ()))
CONTRACT_MID = (((1,), (0,)), ((), ()))
FACTOR = HEAD_DIM ** (-0.5) * LOG2E


def soft(queries, keys, values, biases=None):
    scores = [
        lax.dot_general(q, k, CONTRACT_LAST, preferred_element_type=jnp.float32)
        for q, k in zip(queries, keys)
    ]
    if biases is not None:
        scores = [score + bias for score, bias in zip(scores, biases)]
    tops = [jnp.max(score, axis=1, keepdims=True) for score in scores]
    weights = [jnp.exp2((score - top) * FACTOR) for score, top in zip(scores, tops)]
    totals = [jnp.sum(weight, axis=1, keepdims=True) for weight in weights]
    contexts = [
        lax.dot_general(w.astype(jnp.bfloat16), v, CONTRACT_MID, preferred_element_type=jnp.float32)
        for w, v in zip(weights, values)
    ]
    return list(zip(tops, totals, contexts))


def aligned(start, size=BLOCK):
    return pl.ds(pl.multiple_of(start, BLOCK), size)


def lane_of(shape):
    return lax.broadcasted_iota(jnp.int32, shape, 1)


def lanes_for(lane, span, head):
    mine = lane == head
    for part in range(1, 6):
        mine = jnp.logical_or(mine, lane == part * span + head)
    return mine


def keep(stats, rows, mine, is_top, top, total):
    stats[rows, :] = jnp.where(mine, jnp.where(is_top, top, total), stats[rows, :])


def pieces(value, span):
    lane = lane_of(value.shape)
    high = value.astype(jnp.bfloat16).astype(jnp.float32)
    middle = (value - high).astype(jnp.bfloat16).astype(jnp.float32)
    low = value - high - middle
    out = jnp.zeros_like(value)
    for part in range(6):
        here = jnp.logical_and(lane >= part * span, lane < (part + 1) * span)
        out = jnp.where(here, (high, middle, low)[part % 3], out)
    return out


def unpieced(value, span, head):
    row = lax.broadcasted_iota(jnp.int32, (value.shape[1], LANES), 0)
    mine = lanes_for(row, span, head)
    is_top = row < 3 * span
    return [
        jnp.dot(
            value,
            jnp.where(jnp.logical_and(mine, side), 1.0, 0.0).astype(jnp.bfloat16),
            preferred_element_type=jnp.float32,
        )
        for side in (is_top, jnp.logical_not(is_top))
    ]


def spare_places(token_count, heads):
    return [
        (token_count + n // heads * SPARE, n % heads * LANES, n * LANES) for n in range(token_count // LANES)
    ]


def spare_rows(token_count, heads):
    return -(-(token_count // LANES) // heads) * SPARE


def near_attention(params, queries, key_rows, value_rows, before, after, tokens, total_blocks):
    token_count, width = queries.shape
    heads = width // HEAD_DIM
    blocks_here = token_count // BLOCK
    window = 3 * BLOCK

    def body(par, query_ref, key_ref, value_ref, before_ref, after_ref, token_ref, out_ref, piece_ref, wide, stats):
        step = pl.program_id(0)
        for side, ref in ((0, key_ref), (1, value_ref)):
            wide[side, 0:BLOCK, :] = before_ref[side]
            wide[side, BLOCK : BLOCK + token_count, :] = ref[...]
            wide[side, BLOCK + token_count : 2 * BLOCK + token_count, :] = after_ref[side]
        place = lax.broadcasted_iota(jnp.int32, (1, window + GLOBAL), 1) // BLOCK
        seq_index = par[0]
        lane = lane_of((BLOCK, LANES))
        mine, is_top = lanes_for(lane, heads, step), lane < 3 * heads

        def some_blocks(turn, _):
            numbers = [turn * NEAR_GROUP + i for i in range(NEAR_GROUP)]
            here = [aligned(number * BLOCK) for number in numbers]
            near = [aligned(number * BLOCK, window) for number in numbers]
            keys, values = (
                [jnp.concatenate([wide[side, rows, :], token_ref[side]], axis=0) for rows in near]
                for side in range(2)
            )
            blocks = [seq_index * blocks_here + number for number in numbers]
            biases = [
                jnp.where(
                    jnp.logical_or(
                        jnp.logical_and(place == 0, block == 0),
                        jnp.logical_and(place == 2, block == total_blocks - 1),
                    ),
                    masked_score,
                    0.0,
                )
                for block in blocks
            ]
            found = soft([query_ref[rows, :] for rows in here], keys, values, biases)
            for rows, block, (top, total, context) in zip(here, blocks, found):
                out_ref[rows, :] = context
                top = jnp.where(block < GLOBAL // BLOCK, masked_score, top)
                keep(stats, rows, mine, is_top, top, total)
            return 0

        lax.fori_loop(0, blocks_here // NEAR_GROUP, some_blocks, 0)

        @pl.when(step == heads - 1)
        def _():
            piece_ref[...] = pieces(stats[...], heads).astype(jnp.bfloat16)

    column = pl.BlockSpec((token_count, HEAD_DIM), lambda h, par: (0, h))
    edge = pl.BlockSpec((2, BLOCK, HEAD_DIM), lambda h, par: (0, 0, h))
    return pl.pallas_call(
        body,
        grid_spec=pltpu.PrefetchScalarGridSpec(
            num_scalar_prefetch=1,
            grid=(heads,),
            in_specs=[column, column, column, edge, edge, pl.BlockSpec((2, GLOBAL, HEAD_DIM), lambda h, par: (0, 0, h))],
            out_specs=[column, pl.BlockSpec((token_count, LANES), lambda h, par: (0, 0))],
            scratch_shapes=[
                pltpu.VMEM((2, token_count + 2 * BLOCK, HEAD_DIM), jnp.bfloat16),
                pltpu.VMEM((token_count, LANES), jnp.float32),
            ],
        ),
        out_shape=[
            jax.ShapeDtypeStruct((token_count, width), jnp.float32),
            jax.ShapeDtypeStruct((token_count, LANES), jnp.bfloat16),
        ],
        compiler_params=pltpu.CompilerParams(dimension_semantics=("arbitrary",)),
        cost_estimate=pl.CostEstimate(
            flops=4 * width * token_count * (window + GLOBAL), bytes_accessed=8 * token_count * width, transcendentals=0
        ),
        name="near",
    )(params, queries, key_rows, value_rows, before, after, tokens)


def column_attention(params, queries, pairs, names):
    width = queries[0].shape[1]
    token_count = pairs[0].shape[1]
    heads = width // HEAD_DIM
    blocks_here = token_count // BLOCK
    column_tokens = len(pairs) * token_count
    asked = RANDOM * BLOCK
    callers = len(queries)
    rows_sent = token_count + spare_rows(token_count, heads)

    def body(par, *rest):
        query_refs = rest[:callers]
        pair_refs = rest[callers : callers + len(pairs)]
        outs = rest[callers + len(pairs) : 2 * callers + len(pairs)]
        buf, stats, sems = rest[2 * callers + len(pairs) :]
        step = pl.program_id(0)
        slot = lax.rem(step, 2)

        def copies(head, into):
            columns = pl.ds(pl.multiple_of(head * HEAD_DIM, HEAD_DIM), HEAD_DIM)
            return [
                pltpu.make_async_copy(
                    ref.at[:, :, columns],
                    buf.at[into, :, aligned(par[names["layer"] + number] * token_count, token_count), :],
                    sems.at[into, number],
                )
                for number, ref in enumerate(pair_refs)
            ]

        def work():
            @pl.when(step == 0)
            def _():
                for copy in copies(0, 0):
                    copy.start()

            @pl.when(step + 1 < heads)
            def _():
                for copy in copies(step + 1, 1 - slot):
                    copy.start()

            for copy in copies(step, slot):
                copy.wait()

            columns = pl.ds(pl.multiple_of(step * HEAD_DIM, HEAD_DIM), HEAD_DIM)
            place = lax.broadcasted_iota(jnp.int32, (1, asked), 1) // BLOCK

            masks = {}
            for count in (BLOCK, GLOBAL):
                lane = lane_of((count, LANES))
                masks[count] = lanes_for(lane, heads, step), lane < 3 * heads

            def store(caller, rows, count, top, total, context):
                outs[caller][rows, columns] = context.astype(jnp.bfloat16)
                keep(stats.at[caller], rows, *masks[count], top, total)

            def some_blocks(turn, _):
                chosen = [(caller, turn * GROUP + i) for i in range(GROUP) for caller in range(callers)]
                here = [aligned(number * BLOCK) for _, number in chosen]
                places_of = [caller * blocks_here + number for caller, number in chosen]
                spots = [
                    [aligned(par[names["spots"] + at * RANDOM + r]) for r in range(RANDOM)] for at in places_of
                ]
                keys, values = (
                    [jnp.concatenate([buf[slot, side, spot, :] for spot in row], axis=0) for row in spots]
                    for side in range(2)
                )
                biases = [
                    jnp.where(place < par[names["counts"] + at], 0.0, masked_score) for at in places_of
                ]
                asked_by = [query_refs[caller][rows, :] for (caller, _), rows in zip(chosen, here)]
                found = soft(asked_by, keys, values, biases)
                for (caller, _), rows, part in zip(chosen, here, found):
                    store(caller, rows, BLOCK, *part)
                return 0

            lax.fori_loop(0, blocks_here // GROUP, some_blocks, 0)

            def ends_of_line(caller):
                @pl.when(par[names["device"] + caller] == 0)
                def _():
                    query = query_refs[caller][0:GLOBAL, :]
                    rows = [slice(n * token_count, (n + 1) * token_count) for n in range(len(pairs))]
                    keys, values = ([buf[slot, side, row, :] for row in rows] for side in range(2))
                    found = soft([query] * len(pairs), keys, values)
                    joint = found[0][0]
                    for part in found[1:]:
                        joint = jnp.maximum(joint, part[0])
                    shares = [jnp.exp2((part[0] - joint) * FACTOR) for part in found]
                    total = sum(part[1] * share for part, share in zip(found, shares))
                    context = sum(part[2] * share for part, share in zip(found, shares))
                    store(caller, slice(0, GLOBAL), GLOBAL, joint, total, context)

            for caller in range(callers):
                if caller % 2:
                    ends_of_line(caller)

                @pl.when(step == heads - 1)
                def _():
                    for row, column, token in spare_places(token_count, heads):
                        part = jnp.transpose(pieces(stats[caller, token : token + LANES, :], heads))
                        outs[caller][row : row + SPARE, column : column + LANES] = part[:SPARE].astype(jnp.bfloat16)

        pl.when(par[names["inner"]] == 1)(work)

    return pl.pallas_call(
        body,
        grid_spec=pltpu.PrefetchScalarGridSpec(
            num_scalar_prefetch=1,
            grid=(heads,),
            in_specs=[pl.BlockSpec((token_count, HEAD_DIM), lambda h, par: (0, h))] * callers
            + [pl.BlockSpec(memory_space=pl.ANY)] * len(pairs),
            out_specs=[pl.BlockSpec((rows_sent, width), lambda h, par: (0, 0))] * callers,
            scratch_shapes=[
                pltpu.VMEM((2, 2, column_tokens, HEAD_DIM), jnp.bfloat16),
                pltpu.VMEM((callers, token_count, LANES), jnp.float32),
                pltpu.SemaphoreType.DMA((2, len(pairs))),
            ],
        ),
        out_shape=[jax.ShapeDtypeStruct((rows_sent, width), jnp.bfloat16)] * callers,
        compiler_params=pltpu.CompilerParams(dimension_semantics=("arbitrary",)),
        cost_estimate=pl.CostEstimate(
            flops=4 * width * token_count * callers * asked, bytes_accessed=4 * column_tokens * width, transcendentals=0
        ),
    )(params, *queries, *pairs)


def merge(params, near, near_lse, inner_pair, outer_pair, first_head, names, head_count):
    token_count = near.shape[0]
    rows_sent, width = inner_pair[0].shape
    heads = width // HEAD_DIM
    quarter = token_count // head_count
    some = inner_pair + outer_pair

    def body(par, near_ref, lse_ref, *rest):
        parts = rest[: len(some)]
        outs = rest[len(some) : -2]
        stats, done = rest[-2:]
        step = pl.program_id(0)

        def join(group):
            @pl.when(step == 0)
            def _():
                for side, number in enumerate(group):
                    for row, column, token in spare_places(token_count, heads):
                        part = parts[number][row : row + SPARE, column : column + LANES].astype(jnp.float32)
                        stats[side, token : token + LANES, :] = jnp.transpose(part)

            columns = pl.ds(pl.multiple_of(step * HEAD_DIM, HEAD_DIM), HEAD_DIM)
            all_heads = near.shape[1] // HEAD_DIM
            found = [unpieced(lse_ref[...], all_heads, first_head + step) + [near_ref[...]]]
            for side, number in enumerate(group):
                context = parts[number][0:token_count, columns].astype(jnp.float32)
                found.append(unpieced(stats[side].astype(jnp.bfloat16), heads, step) + [context])
            top = jnp.maximum(jnp.maximum(found[0][0], found[1][0]), found[2][0])
            shares = [jnp.exp2((part[0] - top) * FACTOR) for part in found]
            total = sum(part[1] * share for part, share in zip(found, shares))
            context = sum(part[2] * share for part, share in zip(found, shares))
            done[...] = (context / total).astype(jnp.bfloat16)

        pl.when(par[names["inner"]] == 1)(lambda: join((0, 1)))
        pl.when(par[names["inner"]] == 0)(lambda: join((2, 3)))
        for number in range(head_count):
            start = jnp.bitwise_xor(par[names["head"]], number) * quarter
            outs[number][...] = done[pl.ds(pl.multiple_of(start, quarter), quarter), :]

    return pl.pallas_call(
        body,
        grid_spec=pltpu.PrefetchScalarGridSpec(
            num_scalar_prefetch=1,
            grid=(heads,),
            in_specs=[
                pl.BlockSpec((token_count, HEAD_DIM), lambda h, par: (0, first_head + h)),
                pl.BlockSpec((token_count, LANES), lambda h, par: (0, 0)),
            ]
            + [pl.BlockSpec((rows_sent, width), lambda h, par: (0, 0))] * len(some),
            out_specs=[pl.BlockSpec((quarter, HEAD_DIM), lambda h, par: (0, h))] * head_count,
            scratch_shapes=[
                pltpu.VMEM((2, token_count, SPARE), jnp.float32),
                pltpu.VMEM((token_count, HEAD_DIM), jnp.bfloat16),
            ],
        ),
        out_shape=[jax.ShapeDtypeStruct((quarter, width), jnp.bfloat16)] * head_count,
        compiler_params=pltpu.CompilerParams(dimension_semantics=("arbitrary",)),
        cost_estimate=pl.CostEstimate(flops=64 * token_count * width, bytes_accessed=8 * token_count * width, transcendentals=0),
    )(params, near, near_lse, *some)


def project(parts, weights, first_row, so_far=None, tile=512):
    rows = parts[0][0].shape[0]
    width = weights[0].shape[1]
    chunks = len(parts[0])
    used = sum(part.shape[1] for part in parts[0])
    sides = len(weights)

    def body(*refs):
        part_refs = refs[: sides * chunks]
        weight_refs = refs[sides * chunks : sides * chunks + sides]
        total = jnp.zeros((rows, tile), jnp.float32) if so_far is None else refs[-2][...]
        for number, weight in enumerate(weight_refs):
            left = [part_refs[number * chunks + c][...] for c in range(chunks)]
            left = jnp.concatenate(left, axis=1) if chunks > 1 else left[0]
            total = total + jnp.dot(left, weight[...], preferred_element_type=jnp.float32)
        refs[-1][...] = total.astype(refs[-1].dtype)

    flat = [part for group in parts for part in group]
    extra = [] if so_far is None else [so_far]
    column = pl.BlockSpec((rows, tile), lambda n: (0, n))
    return pl.pallas_call(
        body,
        grid=(width // tile,),
        in_specs=[pl.BlockSpec(part.shape, lambda n: (0, 0)) for part in flat]
        + [pl.BlockSpec((pl.Element(used), pl.Element(tile)), lambda n: (first_row, n * tile))] * sides
        + [column] * len(extra),
        out_specs=column,
        out_shape=jax.ShapeDtypeStruct((rows, width), jnp.float32 if so_far is None else jnp.bfloat16),
        compiler_params=pltpu.CompilerParams(dimension_semantics=("arbitrary",)),
        cost_estimate=pl.CostEstimate(
            flops=2 * rows * used * sides * width, bytes_accessed=2 * used * sides * width, transcendentals=0
        ),
    )(*flat, *weights, *extra)


def local_columns(queries, key_rows, value_rows, random_owner, random_local, output_weight):
    seq_count, head_count = lax.axis_size("seq"), lax.axis_size("head")
    token_count, width_here = queries.shape
    heads_here = width_here // HEAD_DIM
    blocks_here = token_count // BLOCK
    seq_index, head_index = lax.axis_index("seq"), lax.axis_index("head")
    layer, side = seq_index // 2, seq_index % 2
    last = LAYERS - 1
    inner = jnp.logical_and(layer > 0, layer < last)
    outer_layer = jnp.where(layer * 2 < last, 0, last)
    mirror = last - layer
    ends = ((0, 1), (last, last - 1))
    to_inner = [(2 * a + x, 2 * b + x) for a, b in ends for x in range(2)]
    to_outer = [(b, a) for a, b in to_inner]
    to_outer_across = [(2 * b + x, 2 * a + 1 - x) for a, b in ends for x in range(2)]
    middle = [(2 * a + x, 2 * (last - a) + x) for _, a in ends for x in range(2)]
    across = [(2 * a + x, 2 * a + 1 - x) for _, a in ends for x in range(2)]

    def move(array, pairs):
        return lax.ppermute(array, "seq", pairs)

    def swap(array, distance):
        return lax.ppermute(array, "head", [(i, i ^ distance) for i in range(head_count)])

    last_block = jnp.stack([key_rows[-BLOCK:], value_rows[-BLOCK:]])
    first_block = jnp.stack([key_rows[:BLOCK], value_rows[:BLOCK]])
    before = move(last_block, [(i, i + 1) for i in range(seq_count - 1)])
    after = move(first_block, [(i + 1, i) for i in range(seq_count - 1)])
    tokens = jnp.stack([key_rows[:GLOBAL], value_rows[:GLOBAL]])
    hops = [[(0, 1)]] + [[(2 * z + x, 2 * z + 2 + x) for x in range(2)] for z in range(LAYERS - 1)]
    for pairs in hops:
        got = move(tokens, pairs)
        reached = jnp.any(jnp.array([b for _, b in pairs]) == seq_index)
        tokens = jnp.where(reached, got, tokens)

    far_weight = swap(output_weight, 2)
    near, near_lse = near_attention(
        seq_index.astype(jnp.int32).reshape(1), queries, key_rows, value_rows, before, after, tokens, seq_count * blocks_here
    )

    parts = [[] for _ in range(head_count)]
    first_head = 0
    moved = []
    for number, size in enumerate(CHUNKS):
        size = heads_here * size // sum(CHUNKS)
        columns = slice(first_head * HEAD_DIM, (first_head + size) * HEAD_DIM)
        pair = jnp.stack([key_rows[:, columns], value_rows[:, columns]])
        query = queries[:, columns]
        if number == 0:
            listed = jnp.concatenate([random_owner, random_local], axis=1).astype(queries.dtype)
            spare = (0, query.shape[1] - 2 * RANDOM)
            query = jnp.concatenate([query, jnp.pad(listed, ((0, 0), spare))], axis=0)
        outer_pair = move(pair, to_inner)
        mirror_pair = move(pair, middle)
        from_outer = move(query, to_inner)
        from_side = move(query, across)
        callers = [query, from_outer, from_side, move(from_outer, across)]
        mirror_outer = move(outer_pair, middle)
        moved.append((first_head, callers, [pair, outer_pair, mirror_pair, mirror_outer]))
        first_head += size
    tables = jnp.stack([asked[token_count:, : 2 * RANDOM] for asked in moved[0][1]]).astype(jnp.int32)
    owners, locals_of = tables[:, :, :RANDOM], tables[:, :, RANDOM:]
    spots = owners // 2 * token_count + locals_of * BLOCK
    here = (owners % 2 == side).astype(jnp.int32)
    rank = jnp.cumsum(here, axis=2) - 1
    packed = [
        jnp.sum(jnp.where(jnp.logical_and(here == 1, rank == r), spots, 0), axis=2) for r in range(RANDOM)
    ]
    outer_device = 2 * outer_layer + side
    head_line = [seq_index, head_index, inner]
    layers = [layer, outer_layer, mirror, last - outer_layer]
    devices = [seq_index, outer_device, seq_index + 1 - 2 * side, outer_device + 1 - 2 * side]
    params = jnp.concatenate(
        [
            jnp.stack([jnp.asarray(v, jnp.int32) for v in head_line + layers + devices]),
            jnp.stack(packed, axis=2).reshape(-1),
            jnp.sum(here, axis=2).reshape(-1),
        ]
    ).astype(jnp.int32)
    names = {"seq": 0, "head": 1, "inner": 2, "layer": 3, "device": 7, "spots": 11}
    names["counts"] = 11 + 4 * blocks_here * RANDOM

    for first, callers, pairs in moved:
        found = column_attention(params, callers, pairs, names)
        inner_pair = [found[0], move(found[2], across)]
        outer_pair = [move(found[1], to_outer), move(found[3], to_outer_across)]
        outs = merge(params, near, near_lse, inner_pair, outer_pair, first, names, head_count)
        for distance, part in enumerate(outs):
            parts[distance].append(swap(part, distance) if distance else part)
    weights = [output_weight, swap(output_weight, 1), far_weight, swap(far_weight, 1)]
    early = project([part[:1] for part in parts], weights, 0)
    return project([part[1:] for part in parts], weights, moved[1][0] * HEAD_DIM, early)


def local(*arrays):
    if lax.axis_size("seq") != 2 * LAYERS:
        return local_exchange(*arrays)
    return local_columns(*arrays)


def solution(mesh):
    in_specs = (
        P("seq", "head"),
        P("seq", "head"),
        P("seq", "head"),
        P("seq", None),
        P("seq", None),
        P("head", None),
    )
    out_specs = P(("seq", "head"), None)
    return jax.shard_map(local, mesh=mesh, in_specs=in_specs, out_specs=out_specs, check_vma=False)
```
